8 devices in a mesh: fsdp: 8 (over z, y, x, core).
Axes of the slice: x: 2, y: 2, z: 1, core: 2. Of those that a mesh axis runs over, the one named last changes fastest.
Arguments:
- tok_ids: int32 [16, 1024], P('fsdp')
- grad_out: bfloat16 [16, 1024, 2048], P('fsdp')
- emb_table: bfloat16 [151936, 2048], P('fsdp')
- norm_gain: bfloat16 [2048], P('fsdp')
- w_query: bfloat16 [2048, 2048], P('fsdp')
- b_query: bfloat16 [2048], P('fsdp')
- w_key: bfloat16 [2048, 2048], P('fsdp')
- b_key: bfloat16 [2048], P('fsdp')
- w_value: bfloat16 [2048, 2048], P('fsdp')
- b_value: bfloat16 [2048], P('fsdp')
- w_out: bfloat16 [2048, 2048], P('fsdp')
Outputs:
- output 1: bfloat16 [16, 1024, 2048], P('fsdp')
- output 2: bfloat16 [151936, 2048], P('fsdp')
- output 3: float32 [2048], P('fsdp')
- output 4: float32 [2048, 2048], P('fsdp')
- output 5: float32 [2048], P('fsdp')
- output 6: float32 [2048, 2048], P('fsdp')
- output 7: float32 [2048], P('fsdp')
- output 8: float32 [2048, 2048], P('fsdp')
- output 9: float32 [2048], P('fsdp')
- output 10: float32 [2048, 2048], P('fsdp')
All inputs are finite; a program needn't handle non-finite values.
Results may differ from the reference program's by a relative error of at most 0.0130164.
Values are sent between devices in bfloat16 or wider.
A program may use at most 1 GiB of HBM per device.

```python
import jax
import jax.numpy as jnp
from jax import lax

VOCAB = 151936
D_MODEL = 2048
HEADS = 16
KV_HEADS = 16
HEAD_DIM = 128
BATCH = 16
SEQ = 1024
HOT_IDS = 4096
ROPE_THETA = 1.0e6
NORM_EPS = 1e-6
MASK_VALUE = -1e30


def draw_ids(key_ids):
    key_pick, key_hot, key_wide = jax.random.split(key_ids, 3)
    pick_hot = jax.random.randint(key_pick, (BATCH, SEQ), 0, 2)
    low_ids = jax.random.randint(key_hot, (BATCH, SEQ), 0, HOT_IDS)
    hot_ids = (low_ids * low_ids) // HOT_IDS
    wide_ids = jax.random.randint(key_wide, (BATCH, SEQ), 0, VOCAB)
    tok_ids = jnp.where(pick_hot == 0, hot_ids, wide_ids).astype(jnp.int32)
    return tok_ids.at[0, SEQ - 1].set(VOCAB - 1)


def setup_inputs(seed: int = 0) -> dict:
    key_list = jax.random.split(jax.random.key(seed), 12)
    q_width = HEADS * HEAD_DIM
    kv_width = KV_HEADS * HEAD_DIM
    in_scale = D_MODEL ** -0.5
    out_scale = q_width ** -0.5

    def normal(key_n, shape):
        return jax.random.normal(key_n, shape, jnp.float32)

    return {
        "tok_ids": draw_ids(key_list[0]),
        "grad_out": normal(key_list[1], (BATCH, SEQ, D_MODEL)).astype(jnp.bfloat16),
        "emb_table": normal(key_list[2], (VOCAB, D_MODEL)).astype(jnp.bfloat16),
        "norm_gain": (1.0 + 0.3 * normal(key_list[3], (D_MODEL,))).astype(jnp.bfloat16),
        "w_query": (in_scale * normal(key_list[4], (D_MODEL, q_width))).astype(jnp.bfloat16),
        "b_query": (0.5 * normal(key_list[5], (q_width,))).astype(jnp.bfloat16),
        "w_key": (in_scale * normal(key_list[6], (D_MODEL, kv_width))).astype(jnp.bfloat16),
        "b_key": (0.5 * normal(key_list[7], (kv_width,))).astype(jnp.bfloat16),
        "w_value": (in_scale * normal(key_list[8], (D_MODEL, kv_width))).astype(jnp.bfloat16),
        "b_value": (0.5 * normal(key_list[9], (kv_width,))).astype(jnp.bfloat16),
        "w_out": (out_scale * normal(key_list[10], (q_width, D_MODEL))).astype(jnp.bfloat16),
    }


def rope_tables():
    half_dim = HEAD_DIM // 2
    inv_freq = jnp.power(ROPE_THETA, -(jnp.arange(half_dim, dtype=jnp.float32) * 2.0 / HEAD_DIM))
    angles = jnp.arange(SEQ, dtype=jnp.float32)[:, None] * inv_freq[None, :]
    angles = jnp.concatenate([angles, angles], axis=-1)
    return jnp.cos(angles)[:, None, :], jnp.sin(angles)[:, None, :]


def rotate(vector, cos_t, sin_t):
    half_dim = HEAD_DIM // 2
    turned = jnp.concatenate([-vector[..., half_dim:], vector[..., :half_dim]], axis=-1)
    return vector * cos_t + turned * sin_t


def block_seq(x_seq, params):
    gain_vec, w_query, b_query, w_key, b_key, w_value, b_value, w_out = params
    cos_t, sin_t = rope_tables()
    q_group = HEADS // KV_HEADS
    inv_rms = lax.rsqrt(jnp.mean(x_seq * x_seq, axis=-1, keepdims=True) + NORM_EPS)
    hidden = (x_seq * inv_rms * gain_vec).astype(jnp.bfloat16).astype(jnp.float32)
    q_lin = jnp.dot(hidden, w_query, preferred_element_type=jnp.float32) + b_query
    k_lin = jnp.dot(hidden, w_key, preferred_element_type=jnp.float32) + b_key
    v_lin = jnp.dot(hidden, w_value, preferred_element_type=jnp.float32) + b_value
    q_rot = rotate(q_lin.reshape(SEQ, HEADS, HEAD_DIM), cos_t, sin_t)
    q_rot = q_rot.astype(jnp.bfloat16).astype(jnp.float32).reshape(SEQ, KV_HEADS, q_group, HEAD_DIM)
    k_rot = rotate(k_lin.reshape(SEQ, KV_HEADS, HEAD_DIM), cos_t, sin_t)
    k_rot = k_rot.astype(jnp.bfloat16).astype(jnp.float32)
    v_val = v_lin.reshape(SEQ, KV_HEADS, HEAD_DIM).astype(jnp.bfloat16).astype(jnp.float32)
    scores = jnp.einsum("qkgd,skd->kgqs", q_rot, k_rot) * (HEAD_DIM ** -0.5)
    causal = jnp.arange(SEQ)[:, None] >= jnp.arange(SEQ)[None, :]
    scores = jnp.where(causal, scores, MASK_VALUE)
    prob_b = jax.nn.softmax(scores, axis=-1).astype(jnp.bfloat16).astype(jnp.float32)
    attn_out = jnp.einsum("kgqs,skd->qkgd", prob_b, v_val).reshape(SEQ, HEADS * HEAD_DIM)
    attn_out = attn_out.astype(jnp.bfloat16).astype(jnp.float32)
    proj_out = jnp.dot(attn_out, w_out, preferred_element_type=jnp.float32)
    return (x_seq + proj_out).astype(jnp.bfloat16)


def reference(tok_ids, grad_out, emb_table, norm_gain, w_query, b_query, w_key, b_key, w_value, b_value, w_out):
    x_all = jnp.take(emb_table, tok_ids, axis=0).astype(jnp.float32)
    params = tuple(weight.astype(jnp.float32) for weight in (norm_gain, w_query, b_query, w_key, b_key, w_value, b_value, w_out))
    seq_step = jax.checkpoint(block_seq)

    def forward(x_in, prm_list):
        return lax.map(lambda x_seq: seq_step(x_seq, prm_list), x_in)

    block_out, pullback = jax.vjp(forward, x_all, params)
    d_x, d_params = pullback(grad_out)
    grad_table = jax.ops.segment_sum(d_x.reshape(-1, D_MODEL), tok_ids.reshape(-1), num_segments=VOCAB)
    grad_table = grad_table.astype(jnp.bfloat16)
    return (block_out, grad_table, d_params[0], d_params[1], d_params[2], d_params[3], d_params[4], d_params[5], d_params[6], d_params[7])
```

```python
import functools

import jax
import jax.numpy as jnp
from jax import lax
from jax.experimental import pallas as pl
from jax.experimental.pallas import tpu as pltpu
from jax.sharding import PartitionSpec as P

HEAD_DIM = 128
ROPE_THETA = 1.0e6
NORM_EPS = 1e-6
MASK_VALUE = -1e30
AXIS = "fsdp"
N_DEV = 8
HOT = 4096
CAP = 192
LANES = 128
BIG = 2**31 - 1
MESH = pl.DeviceIdType.MESH
BLOCK_Q = 256
ROW_BLOCK = 128
VMEM_MAX = 60 * 1024 * 1024


def dot_nn(a, b):
    return lax.dot_general(a, b, (((1,), (0,)), ((), ())), preferred_element_type=jnp.float32)


def dot_nt(a, b):
    return lax.dot_general(a, b, (((1,), (1,)), ((), ())), preferred_element_type=jnp.float32)


def attn_kernel(q_ref, k_ref, v_ref, do_ref, cos_ref, sin_ref, bq_ref, bk_ref,
                o_ref, dq_ref, dk_ref, dv_ref, gb_ref, qs, ks, dkt, dvt):
    seq_len = q_ref.shape[0]
    score_scale = HEAD_DIM ** -0.5
    cos_t = cos_ref[...]
    sin_t = sin_ref[...]
    half = HEAD_DIM // 2
    q_lin = q_ref[...] + bq_ref[...]
    qs[...] = (q_lin * cos_t + pltpu.roll(q_lin, half, 1) * sin_t).astype(jnp.bfloat16)
    k_lin = k_ref[...] + bk_ref[...]
    ks[...] = (k_lin * cos_t + pltpu.roll(k_lin, half, 1) * sin_t).astype(jnp.bfloat16)
    row_i = lax.broadcasted_iota(jnp.int32, (BLOCK_Q, BLOCK_Q), 0)
    col_i = lax.broadcasted_iota(jnp.int32, (BLOCK_Q, BLOCK_Q), 1)
    causal = row_i >= col_i
    n_blocks = seq_len // BLOCK_Q
    gbq = jnp.zeros((1, HEAD_DIM), jnp.float32)
    for blk in reversed(range(n_blocks)):
        lo = blk * BLOCK_Q
        width = lo + BLOCK_Q
        q_b = qs[pl.ds(lo, BLOCK_Q), :]
        do_b = do_ref[pl.ds(lo, BLOCK_Q), :]
        k_all = ks[pl.ds(0, width), :]
        v_all = v_ref[pl.ds(0, width), :]
        scores = dot_nt(q_b, k_all) * score_scale
        tail = jnp.where(causal, scores[:, lo:], MASK_VALUE)
        scores = jnp.concatenate([scores[:, :lo], tail], axis=1) if lo else tail
        top = jnp.max(scores, axis=1, keepdims=True)
        prob = jnp.exp(scores - top)
        prob = prob * (1.0 / jnp.sum(prob, axis=1, keepdims=True))
        prob_b = prob.astype(jnp.bfloat16)
        o_ref[pl.ds(lo, BLOCK_Q), :] = dot_nn(prob_b, v_all).astype(jnp.bfloat16)
        d_prob = dot_nt(do_b, v_all)
        inner = jnp.sum(d_prob * prob, axis=1, keepdims=True)
        d_score = ((prob * (d_prob - inner)) * score_scale).astype(jnp.bfloat16)
        d_q = dot_nn(d_score, k_all)
        scaled = d_q * sin_ref[pl.ds(lo, BLOCK_Q), :]
        d_q = d_q * cos_ref[pl.ds(lo, BLOCK_Q), :] + pltpu.roll(scaled, half, 1)
        gbq = gbq + jnp.sum(d_q, axis=0, keepdims=True)
        dq_ref[pl.ds(lo, BLOCK_Q), :] = d_q.astype(jnp.bfloat16)
        dv_part = dot_nn(do_b.T, prob_b)
        dk_part = dot_nn(q_b.T, d_score)
        if blk == n_blocks - 1:
            dvt[...] = dv_part
            dkt[...] = dk_part
        else:
            dvt[:, pl.ds(0, width)] += dv_part
            dkt[:, pl.ds(0, width)] += dk_part
    d_v = dvt[...].T
    d_k = dkt[...].T
    d_k = d_k * cos_t + pltpu.roll(d_k * sin_t, half, 1)
    dv_ref[...] = d_v.astype(jnp.bfloat16)
    dk_ref[...] = d_k.astype(jnp.bfloat16)
    gb_ref[0, 0:1, :] = gbq
    gb_ref[0, 1:2, :] = jnp.sum(d_k, axis=0, keepdims=True)
    gb_ref[0, 2:3, :] = jnp.sum(d_v, axis=0, keepdims=True)
    gb_ref[0, 3:8, :] = jnp.zeros((5, HEAD_DIM), jnp.float32)


def attention(q_lin, k_lin, v_val, d_attn, b_q, b_k, seq_len):
    tokens, width = q_lin.shape
    n_seq, n_heads = tokens // seq_len, width // HEAD_DIM
    half = HEAD_DIM // 2
    inv_freq = jnp.power(ROPE_THETA, -(jnp.arange(half, dtype=jnp.float32) * 2.0 / HEAD_DIM))
    angles = jnp.arange(seq_len, dtype=jnp.float32)[:, None] * inv_freq[None, :]
    cos_t = jnp.concatenate([jnp.cos(angles)] * 2, axis=-1)
    sin_t = jnp.concatenate([-jnp.sin(angles), jnp.sin(angles)], axis=-1)
    tile = pl.BlockSpec((seq_len, HEAD_DIM), lambda s, h: (s, h))
    table = pl.BlockSpec((seq_len, HEAD_DIM), lambda s, h: (0, 0))
    bias = pl.BlockSpec((1, HEAD_DIM), lambda s, h: (0, h))
    act = jax.ShapeDtypeStruct((tokens, width), jnp.bfloat16)
    pairs = n_seq * n_heads * seq_len * seq_len
    return pl.pallas_call(
        attn_kernel,
        grid=(n_seq, n_heads),
        in_specs=[tile, tile, tile, tile, table, table, bias, bias],
        out_specs=[tile, tile, tile, tile, pl.BlockSpec((1, 8, HEAD_DIM), lambda s, h: (s, 0, h))],
        out_shape=[act, act, act, act, jax.ShapeDtypeStruct((n_seq, 8, width), jnp.float32)],
        scratch_shapes=[
            pltpu.VMEM((seq_len, HEAD_DIM), jnp.bfloat16),
            pltpu.VMEM((seq_len, HEAD_DIM), jnp.bfloat16),
            pltpu.VMEM((HEAD_DIM, seq_len), jnp.float32),
            pltpu.VMEM((HEAD_DIM, seq_len), jnp.float32),
        ],
        compiler_params=pltpu.CompilerParams(
            dimension_semantics=("arbitrary", "arbitrary"), vmem_limit_bytes=VMEM_MAX),
        cost_estimate=pl.CostEstimate(
            flops=6 * 2 * HEAD_DIM * pairs, bytes_accessed=24 * tokens * width, transcendentals=pairs),
        name="attn_fwd_bwd",
    )(q_lin, k_lin, v_val, d_attn, cos_t, sin_t, b_q.astype(jnp.float32)[None], b_k.astype(jnp.float32)[None])


def block_fwd_bwd(x_rows, grad_out, seq_len, gain_vec, w_query, b_query, w_key, b_key, w_value, b_value, w_out):
    f32 = jnp.float32
    x_full = x_rows.astype(f32)
    inv_rms = lax.rsqrt(jnp.mean(x_full * x_full, axis=-1, keepdims=True) + NORM_EPS)
    x_norm = x_full * inv_rms
    gain_f = gain_vec.astype(f32)
    hidden = (x_norm * gain_f).astype(jnp.bfloat16)
    d_attn = dot_nt(grad_out, w_out).astype(jnp.bfloat16)
    q_lin = dot_nn(hidden, w_query)
    k_lin = dot_nn(hidden, w_key)
    v_val = (dot_nn(hidden, w_value) + b_value.astype(f32)).astype(jnp.bfloat16)
    attn_b, dq_b, dk_b, dv_b, grad_b = attention(q_lin, k_lin, v_val, d_attn, b_query, b_key, seq_len)
    block_out = (x_full + dot_nn(attn_b, w_out)).astype(jnp.bfloat16)
    tn = (((0,), (0,)), ((), ()))
    grad_wo = lax.dot_general(attn_b, grad_out, tn, preferred_element_type=f32)
    d_hidden = dot_nt(dq_b, w_query) + dot_nt(dk_b, w_key) + dot_nt(dv_b, w_value)
    grad_gain = jnp.sum(d_hidden * x_norm, axis=0)
    d_norm = d_hidden * gain_f
    d_x = grad_out.astype(f32) + inv_rms * (d_norm - x_norm * jnp.mean(d_norm * x_norm, axis=-1, keepdims=True))
    grad_wq = lax.dot_general(hidden, dq_b, tn, preferred_element_type=f32)
    grad_wk = lax.dot_general(hidden, dk_b, tn, preferred_element_type=f32)
    grad_wv = lax.dot_general(hidden, dv_b, tn, preferred_element_type=f32)
    grad_b = jnp.sum(grad_b, axis=0)
    vecs = (grad_gain, grad_b[0], grad_b[1], grad_b[2])
    return block_out, d_x, (grad_wq, grad_wk, grad_wv, grad_wo), vecs


def barrier_all(me):
    barrier = pltpu.get_barrier_semaphore()
    for step in range(1, N_DEV):
        pl.semaphore_signal(barrier, inc=1, device_id=(jnp.bitwise_xor(me, step),), device_id_type=MESH)
    pl.semaphore_wait(barrier, N_DEV - 1)


LOOK_CHUNK = 128
LOOK_N = HOT // 2 // LOOK_CHUNK


def lookup_kernel(cold_ref, _, rows_ref, recv_sem, link_sem, mate_sem, c_send, c_recv, l_sem):
    me = lax.axis_index(AXIS)
    chip, core = me // 2, me % 2
    barrier_all(me)
    own = pltpu.make_async_copy(cold_ref.at[me], rows_ref.at[pl.ds(HOT + me * CAP, CAP)], l_sem)
    own.start()

    def cold_copy(step):
        peer = jnp.bitwise_xor(me, step)
        return pltpu.make_async_remote_copy(
            src_ref=cold_ref.at[peer], dst_ref=rows_ref.at[pl.ds(HOT + me * CAP, CAP)],
            send_sem=c_send.at[step - 1], recv_sem=c_recv.at[step - 1],
            device_id=(peer,), device_id_type=MESH)

    def piece(part, k):
        return rows_ref.at[pl.ds(part * (HOT // 2) + k * LOOK_CHUNK, LOOK_CHUNK)]

    def link_copy(part, k, target):
        return pltpu.make_async_remote_copy(
            src_ref=piece(part, k), dst_ref=piece(part, k), send_sem=link_sem.at[part, k],
            recv_sem=recv_sem.at[part, k], device_id=(target,), device_id_type=MESH)

    def mate_copy(part, k):
        return pltpu.make_async_remote_copy(
            src_ref=piece(part, k), dst_ref=piece(part, k), send_sem=mate_sem.at[part, k],
            recv_sem=recv_sem.at[part, k], device_id=(jnp.bitwise_xor(me, 1),), device_id_type=MESH)

    place = [
        jnp.where(chip == 0, 0, jnp.where(chip == 1, 1, jnp.where(chip == 3, 2, 3))),
        jnp.where(chip == 0, 0, jnp.where(chip == 2, 1, jnp.where(chip == 3, 2, 3))),
    ]
    target = [
        2 * jnp.where(chip == 0, 1, jnp.where(chip == 1, 3, 2)),
        2 * jnp.where(chip == 0, 2, jnp.where(chip == 2, 3, 1)),
    ]

    def stage(step, carry):
        for part in range(2):
            k = step - place[part]
            live = (k >= 0) & (k < LOOK_N)

            @pl.when(live & (me != 0))
            def _():
                mate_copy(part, k).wait_recv()

            @pl.when(live & (core == 0) & (place[part] < 3))
            def _():
                link_copy(part, k, target[part]).start()

            @pl.when(live & (core == 0))
            def _():
                mate_copy(part, k).start()
        return carry

    for step in range(1, N_DEV):
        cold_copy(step).start()
    lax.fori_loop(0, LOOK_N + 3, stage, 0)

    def drain(k, carry):
        for part in range(2):
            @pl.when((core == 0) & (place[part] < 3))
            def _():
                link_copy(part, k, target[part]).wait_send()

            @pl.when(core == 0)
            def _():
                mate_copy(part, k).wait_send()
        return carry

    lax.fori_loop(0, LOOK_N, drain, 0)
    for step in range(1, N_DEV):
        cold_copy(step).wait()
    own.wait()


def lookup_exchange(cold_send, rows_in):
    any_spec = pl.BlockSpec(memory_space=pl.ANY)
    dma = pltpu.SemaphoreType.DMA
    return pl.pallas_call(
        lookup_kernel,
        out_shape=jax.ShapeDtypeStruct(rows_in.shape, rows_in.dtype),
        in_specs=[any_spec, any_spec],
        out_specs=any_spec,
        scratch_shapes=[dma((2, LOOK_N)), dma((2, LOOK_N)), dma((2, LOOK_N)), dma((N_DEV - 1,)), dma((N_DEV - 1,)), dma],
        input_output_aliases={1: 0},
        compiler_params=pltpu.CompilerParams(collective_id=0, has_side_effects=True),
        name="lookup_exchange",
    )(cold_send, rows_in)


def pick_kernel(idx_ref, rows_ref, out_ref):
    base = pl.program_id(0) * out_ref.shape[0]

    def body(step, carry):
        for j in range(8):
            i = step * 8 + j
            out_ref[i] = rows_ref[idx_ref[base + i]]
        return carry

    lax.fori_loop(0, out_ref.shape[0] // 8, body, 0)


def pick_rows(idx, rows, block):
    count = idx.shape[0]
    tail = rows.shape[1:]
    zeros = (0,) * len(tail)
    return pl.pallas_call(
        pick_kernel,
        grid_spec=pltpu.PrefetchScalarGridSpec(
            num_scalar_prefetch=1,
            grid=(count // block,),
            in_specs=[pl.BlockSpec(rows.shape, lambda i, s: (0,) + zeros, pipeline_mode=pl.Buffered(1))],
            out_specs=pl.BlockSpec((block,) + tail, lambda i, s: (i,) + zeros),
        ),
        out_shape=jax.ShapeDtypeStruct((count,) + tail, rows.dtype),
        compiler_params=pltpu.CompilerParams(dimension_semantics=("arbitrary",), vmem_limit_bytes=VMEM_MAX),
        name="pick_rows",
    )(idx, rows)


def take2d_kernel(idx_ref, rows_ref, out_ref):
    base = pl.program_id(0) * out_ref.shape[0]

    def body(step, carry):
        for j in range(8):
            i = step * 8 + j
            out_ref[pl.ds(i, 1), :] = rows_ref[pl.ds(idx_ref[base + i], 1), :]
        return carry

    lax.fori_loop(0, out_ref.shape[0] // 8, body, 0)


def take2d(idx, rows, block):
    count = idx.shape[0]
    width = rows.shape[1]
    return pl.pallas_call(
        take2d_kernel,
        grid_spec=pltpu.PrefetchScalarGridSpec(
            num_scalar_prefetch=1,
            grid=(count // block,),
            in_specs=[pl.BlockSpec(rows.shape, lambda i, s: (0, 0), pipeline_mode=pl.Buffered(1))],
            out_specs=pl.BlockSpec((block, width), lambda i, s: (i, 0)),
        ),
        out_shape=jax.ShapeDtypeStruct((count, width), rows.dtype),
        compiler_params=pltpu.CompilerParams(dimension_semantics=("arbitrary",), vmem_limit_bytes=VMEM_MAX),
        name="take_rows",
    )(idx, rows)


def seg_sum_kernel(key_ref, off_ref, mine_ref, mate_ref, out_ref, src, sem):
    blk = pl.program_id(0)
    count = mine_ref.shape[0]

    @pl.when(blk == 0)
    def _():
        first = pltpu.make_async_copy(mine_ref, src.at[pl.ds(0, count)], sem.at[0])
        second = pltpu.make_async_copy(mate_ref, src.at[pl.ds(count, count)], sem.at[1])
        first.start()
        second.start()
        first.wait()
        second.wait()

    out_ref[...] = jnp.zeros_like(out_ref)

    def body(e, carry):
        key = key_ref[e]
        row = lax.shift_right_logical(key, 12) - blk * ROW_BLOCK
        tok = jnp.bitwise_and(key, 4095)
        out_ref[pl.ds(row, 1), :] += src[pl.ds(tok, 1), :]
        return carry

    lax.fori_loop(off_ref[blk], off_ref[blk + 1], body, 0)


def seg_sum(keys, offs, dx_mine, dx_mate, n_rows):
    tokens, width = dx_mine.shape
    any_spec = pl.BlockSpec(memory_space=pl.ANY)
    return pl.pallas_call(
        seg_sum_kernel,
        grid_spec=pltpu.PrefetchScalarGridSpec(
            num_scalar_prefetch=2,
            grid=(n_rows // ROW_BLOCK,),
            in_specs=[any_spec, any_spec],
            out_specs=pl.BlockSpec((ROW_BLOCK, width), lambda i, a, b: (i, 0)),
            scratch_shapes=[pltpu.VMEM((2 * tokens, width), jnp.float32), pltpu.SemaphoreType.DMA((2,))],
        ),
        out_shape=jax.ShapeDtypeStruct((n_rows, width), jnp.float32),
        compiler_params=pltpu.CompilerParams(dimension_semantics=("arbitrary",), vmem_limit_bytes=VMEM_MAX),
        name="hot_seg_sum",
    )(keys, offs, dx_mine, dx_mate)


RED_CHUNK = 64
RED_N = HOT // 2 // RED_CHUNK


def reduce_kernel(part_ref, cold_ref, vec_ref, hot_ref, crecv_ref, vrecv_ref,
                  local, incoming, load_sem, send_sem, recv_sem, out_sem, c_send, c_recv, v_send, v_recv, l_sem):
    me = lax.axis_index(AXIS)
    chip, core = me // 2, me % 2
    mid = jnp.where(core == 0, 1, 2)
    first = 3 - mid
    place = jnp.where(chip == first, 0, jnp.where(chip == 3, 1, jnp.where(chip == mid, 2, 3)))
    nxt = jnp.where(chip == first, 3, jnp.where(chip == 3, mid, 0))
    target = nxt * 2 + core

    def rows(k):
        return pl.ds(k * RED_CHUNK, RED_CHUNK)

    def load(k):
        return pltpu.make_async_copy(part_ref.at[rows(k)], local.at[rows(k)], load_sem.at[k])

    def send(k):
        return pltpu.make_async_remote_copy(
            src_ref=local.at[rows(k)], dst_ref=incoming.at[rows(k)], send_sem=send_sem.at[k],
            recv_sem=recv_sem.at[k], device_id=(target,), device_id_type=MESH)

    def put_own(k):
        return pltpu.make_async_copy(local.at[rows(k)], hot_ref.at[rows(k)], send_sem.at[k])

    def put_far(k):
        return pltpu.make_async_remote_copy(
            src_ref=local.at[rows(k)], dst_ref=hot_ref.at[pl.ds(HOT // 2 + k * RED_CHUNK, RED_CHUNK)],
            send_sem=send_sem.at[k], recv_sem=out_sem.at[k], device_id=(jnp.bitwise_xor(me, 1),), device_id_type=MESH)

    def cold_copy(step):
        peer = jnp.bitwise_xor(me, step)
        return pltpu.make_async_remote_copy(
            src_ref=cold_ref.at[peer], dst_ref=crecv_ref.at[me],
            send_sem=c_send.at[step - 1], recv_sem=c_recv.at[step - 1],
            device_id=(peer,), device_id_type=MESH)

    def vec_copy(step):
        peer = jnp.bitwise_xor(me, step)
        return pltpu.make_async_remote_copy(
            src_ref=vec_ref.at[peer], dst_ref=vrecv_ref.at[me],
            send_sem=v_send.at[step - 1], recv_sem=v_recv.at[step - 1],
            device_id=(peer,), device_id_type=MESH)

    def start_load(k, carry):
        load(k).start()
        return carry

    lax.fori_loop(0, RED_N, start_load, 0)
    barrier_all(me)
    own_c = pltpu.make_async_copy(cold_ref.at[me], crecv_ref.at[me], l_sem.at[0])
    own_v = pltpu.make_async_copy(vec_ref.at[me], vrecv_ref.at[me], l_sem.at[1])
    own_c.start()
    own_v.start()
    for step in range(1, N_DEV):
        vec_copy(step).start()
    for step in range(1, N_DEV):
        cold_copy(step).start()

    def stage(k, carry):
        @pl.when(k < RED_N)
        def _():
            load(k).wait()

        @pl.when((k < RED_N) & (place > 0))
        def _():
            send(k).wait_recv()
            local[rows(k), :] += incoming[rows(k), :]

        @pl.when((k >= 1) & (place < 3))
        def _():
            send(k - 1).start()

        @pl.when((k >= 1) & (me == 0))
        def _():
            put_own(k - 1).start()

        @pl.when((k >= 1) & (me == 1))
        def _():
            put_far(k - 1).start()
        return carry

    lax.fori_loop(0, RED_N + 1, stage, 0)

    def drain(k, carry):
        @pl.when(place < 3)
        def _():
            send(k).wait_send()

        @pl.when(me == 0)
        def _():
            put_own(k).wait()
            put_far(k).wait_recv()

        @pl.when(me == 1)
        def _():
            put_far(k).wait_send()
        return carry

    lax.fori_loop(0, RED_N, drain, 0)
    for step in range(1, N_DEV):
        vec_copy(step).wait()
        cold_copy(step).wait()
    own_c.wait()
    own_v.wait()


def grad_exchange(part, cold_send, vecs):
    any_spec = pl.BlockSpec(memory_space=pl.ANY)
    dma = pltpu.SemaphoreType.DMA
    width = part.shape[1]
    peers = dma((N_DEV - 1,))
    return pl.pallas_call(
        reduce_kernel,
        out_shape=[
            jax.ShapeDtypeStruct((HOT, width), jnp.float32),
            jax.ShapeDtypeStruct(cold_send.shape, cold_send.dtype),
            jax.ShapeDtypeStruct(vecs.shape, vecs.dtype),
        ],
        in_specs=[any_spec] * 3,
        out_specs=[any_spec] * 3,
        scratch_shapes=[
            pltpu.VMEM(part.shape, jnp.float32), pltpu.VMEM(part.shape, jnp.float32),
            dma((RED_N,)), dma((RED_N,)), dma((RED_N,)), dma((RED_N,)), peers, peers, peers, peers, dma((2,)),
        ],
        compiler_params=pltpu.CompilerParams(
            collective_id=1, has_side_effects=True, vmem_limit_bytes=VMEM_MAX),
        name="grad_exchange",
    )(part, cold_send, vecs)


def table_kernel(key_ref, off_ref, n_hot_ref, src_ref, hot_ref, out_ref, acc):
    blk = pl.program_id(0)
    is_hot = blk < n_hot_ref[0]

    @pl.when(is_hot)
    def _():
        acc[...] = hot_ref[...]

    @pl.when(jnp.logical_not(is_hot))
    def _():
        acc[...] = jnp.zeros_like(acc)

    def body(e, carry):
        key = key_ref[e]
        row = lax.shift_right_logical(key, 11) - blk * ROW_BLOCK
        idx = jnp.bitwise_and(key, 2047)
        acc[pl.ds(row, 1), :] += src_ref[pl.ds(idx, 1), :]
        return carry

    lax.fori_loop(off_ref[blk], off_ref[blk + 1], body, 0)
    out_ref[...] = acc[...].astype(out_ref.dtype)


def build_table(keys, offs, n_hot, src, hot, n_rows):
    width = src.shape[1]

    def hot_index(i, k, o, n):
        return (jnp.minimum(i, jnp.maximum(n[0] - 1, 0)), 0)

    return pl.pallas_call(
        table_kernel,
        grid_spec=pltpu.PrefetchScalarGridSpec(
            num_scalar_prefetch=3,
            grid=(pl.cdiv(n_rows, ROW_BLOCK),),
            in_specs=[
                pl.BlockSpec(src.shape, lambda i, k, o, n: (0, 0), pipeline_mode=pl.Buffered(1)),
                pl.BlockSpec((ROW_BLOCK, width), hot_index),
            ],
            out_specs=pl.BlockSpec((ROW_BLOCK, width), lambda i, k, o, n: (i, 0)),
            scratch_shapes=[pltpu.VMEM((ROW_BLOCK, width), jnp.float32)],
        ),
        out_shape=jax.ShapeDtypeStruct((n_rows, width), jnp.bfloat16),
        compiler_params=pltpu.CompilerParams(dimension_semantics=("arbitrary",), vmem_limit_bytes=VMEM_MAX),
        name="build_table",
    )(keys, offs, n_hot, src, hot)


def fast_lookup(all_ids, own_ids, table_part, me):
    rows_dev, width = table_part.shape
    tokens = own_ids.shape[0]
    first_row = me * rows_dev
    t_idx = jnp.arange(tokens, dtype=jnp.int32)
    mine = (all_ids >= HOT) & (all_ids >= first_row) & (all_ids < first_row + rows_dev)
    key = jnp.where(mine, t_idx[None, :] * 32768 + (all_ids - first_row), BIG)
    key = lax.sort(key, dimension=1)[:, :CAP]
    asked = key != BIG
    ask_row = jnp.where(asked, jnp.bitwise_and(key, 32767), 0)
    send = jnp.take(table_part, ask_row.reshape(-1), axis=0, mode="clip")
    tiles = (width // LANES, LANES)
    send = send.reshape((N_DEV, CAP) + tiles)
    rows_in = jnp.pad(table_part[:HOT].reshape((HOT,) + tiles), ((0, N_DEV * CAP), (0, 0), (0, 0)))
    rows_all = lookup_exchange(send, rows_in)
    owners = own_ids // rows_dev
    hit = (owners[None, :] == jnp.arange(N_DEV, dtype=jnp.int32)[:, None]) & (own_ids >= HOT)[None, :]
    place = jnp.cumsum(hit.astype(jnp.int32), axis=1) - 1 + jnp.arange(N_DEV, dtype=jnp.int32)[:, None] * CAP
    slot = jnp.sum(jnp.where(hit, place, 0), axis=0)
    idx = jnp.where(own_ids >= HOT, HOT + slot, own_ids)
    x_rows = pick_rows(idx, rows_all, 256).reshape(tokens, width)
    slot_tok = lax.sort(jnp.where(hit, t_idx[None, :], BIG), dimension=1)[:, :CAP]
    slot_tok = jnp.where(slot_tok == BIG, 0, slot_tok).reshape(-1)
    src = jnp.arange(N_DEV * CAP, dtype=jnp.int32).reshape(N_DEV, CAP)
    owner_keys = lax.sort(jnp.where(asked, ask_row * 2048 + src, BIG).reshape(-1))
    return x_rows, slot_tok, owner_keys


def block_offsets(keys, n_blocks, shift):
    edges = jnp.arange(n_blocks + 1, dtype=jnp.int32) * (ROW_BLOCK << shift)
    return jnp.sum(keys[None, :] < edges[:, None], axis=1).astype(jnp.int32)


def fast_table_grad(all_ids, own_ids, d_x, vecs, slot_tok, owner_keys, me, rows_dev):
    tokens, width = d_x.shape
    mate_of = [(i, i ^ 1) for i in range(N_DEV)]
    dx_mate = lax.ppermute(d_x, AXIS, mate_of)
    mate_ids = lax.dynamic_index_in_dim(all_ids, jnp.bitwise_xor(me, 1), 0, keepdims=False)
    pair_ids = jnp.concatenate([own_ids, mate_ids])
    base = (me % 2) * (HOT // 2)
    inside = (pair_ids >= base) & (pair_ids < base + HOT // 2)
    keys = jnp.where(inside, (pair_ids - base) * 4096 + jnp.arange(2 * tokens, dtype=jnp.int32), BIG)
    keys = lax.sort(keys)
    part = seg_sum(keys, block_offsets(keys, HOT // 2 // ROW_BLOCK, 12), d_x, dx_mate, HOT // 2)
    cold = take2d(slot_tok, d_x, 192).reshape(N_DEV, CAP, width)
    hot, recv, vec_recv = grad_exchange(part, cold, vecs)
    n_hot = jnp.where(me == 0, HOT // ROW_BLOCK, 0).astype(jnp.int32)[None]
    offs = block_offsets(owner_keys, pl.cdiv(rows_dev, ROW_BLOCK), 11)
    grad_part = build_table(owner_keys, offs, n_hot, recv.reshape(N_DEV * CAP, width), hot, rows_dev)
    return grad_part, jnp.sum(vec_recv, axis=0)


def slow_lookup(all_ids, table_part, me):
    rows_dev = table_part.shape[0]
    local_idx = all_ids - me * rows_dev
    is_owned = (local_idx >= 0) & (local_idx < rows_dev)
    looked = jnp.take(table_part, jnp.where(is_owned, local_idx, 0), axis=0)
    looked = jnp.where(is_owned[..., None], looked, jnp.zeros((), jnp.bfloat16))
    return lax.psum_scatter(looked, AXIS, scatter_dimension=0)


def slow_table_grad(all_ids, d_x, me, rows_dev):
    local_idx = all_ids - me * rows_dev
    is_owned = (local_idx >= 0) & (local_idx < rows_dev)
    all_dx = lax.all_gather(d_x, AXIS)
    seg_idx = jnp.where(is_owned, local_idx, rows_dev)
    grad_part = jax.ops.segment_sum(all_dx.reshape(-1, d_x.shape[-1]), seg_idx.reshape(-1), num_segments=rows_dev)
    return grad_part.astype(jnp.bfloat16)


def solution(mesh):
    row_spec = P(AXIS, None)
    vec_spec = P(AXIS)
    act_spec = P(AXIS, None, None)
    weight_specs = (vec_spec, row_spec, vec_spec, row_spec, vec_spec, row_spec, vec_spec, row_spec)
    in_specs = (row_spec, act_spec, row_spec) + weight_specs
    out_specs = (act_spec, row_spec) + weight_specs

    def run(fast, tok_ids, all_ids, grad_out, table_part, gain_part, wq_part, bq_part, wk_part, bk_part, wv_part, bv_part, wo_part):
        me = lax.axis_index(AXIS)
        rows_dev, width = table_part.shape
        n_seq, seq_len = tok_ids.shape
        own_ids = tok_ids.reshape(-1)

        def whole(part):
            return lax.all_gather(part, AXIS, axis=0, tiled=True)

        vec_parts = jnp.stack([gain_part, bq_part, bk_part, bv_part])
        vec_full = lax.all_gather(vec_parts, AXIS, axis=1, tiled=True)
        wo_full, wq_full, wk_full, wv_full = whole(wo_part), whole(wq_part), whole(wk_part), whole(wv_part)
        if fast:
            x_rows, slot_tok, owner_keys = fast_lookup(all_ids, own_ids, table_part, me)
        else:
            x_rows = slow_lookup(all_ids, table_part, me)
        grad_flat = grad_out.reshape(-1, width)
        block_out, d_x, w_grads, vecs = block_fwd_bwd(
            x_rows, grad_flat, seq_len, vec_full[0], wq_full, vec_full[1], wk_full, vec_full[2], wv_full, vec_full[3], wo_full)
        reduced = tuple(lax.psum_scatter(g, AXIS, scatter_dimension=0, tiled=True) for g in w_grads)
        part_w = gain_part.shape[0]
        vecs = jnp.stack(vecs).reshape(4, N_DEV, part_w).transpose(1, 0, 2)
        if fast:
            vecs = jnp.pad(vecs, ((0, 0), (0, 4), (0, 0)))
            grad_part, vec_sum = fast_table_grad(all_ids, own_ids, d_x, vecs, slot_tok, owner_keys, me, rows_dev)
        else:
            grad_part = slow_table_grad(all_ids, d_x, me, rows_dev)
            vec_sum = lax.psum_scatter(vecs, AXIS, scatter_dimension=0)
        gq, gk, gv, go = reduced
        return (block_out.reshape(grad_out.shape), grad_part, vec_sum[0], gq, vec_sum[1], gk, vec_sum[2], gv, vec_sum[3], go)

    def device_step(tok_ids, grad_out, table_part, *weights):
        rows_dev = table_part.shape[0]
        all_ids = lax.all_gather(tok_ids.reshape(-1), AXIS)
        owners = jnp.where(all_ids >= HOT, all_ids // rows_dev, -1)
        counts = jnp.sum((owners[None] == jnp.arange(N_DEV, dtype=jnp.int32)[:, None, None]).astype(jnp.int32), axis=-1)
        fits = jnp.max(counts) <= CAP
        args = (tok_ids, all_ids, grad_out, table_part) + weights
        return lax.cond(fits, functools.partial(run, True), functools.partial(run, False), *args)

    return jax.shard_map(device_step, mesh=mesh, in_specs=in_specs, out_specs=out_specs, check_vma=False)
```

```python
import functools

import jax
import jax.numpy as jnp
from jax import lax
from jax.experimental import pallas as pl
from jax.experimental.pallas import tpu as pltpu
from jax.sharding import PartitionSpec as P

HEAD_DIM = 128
ROPE_THETA = 1.0e6
NORM_EPS = 1e-6
MASK_VALUE = -1e30
AXIS = "fsdp"
N_DEV = 8
HOT = 4096
CAP = 176
MORE = 32
LANES = 128
BIG = 2**31 - 1
MESH = pl.DeviceIdType.MESH
BLOCK_Q = 256
GROUPS = 4
ROW_BLOCK = 128
VMEM_MAX = 60 * 1024 * 1024


def dot_nn(a, b):
    return lax.dot_general(a, b, (((1,), (0,)), ((), ())), preferred_element_type=jnp.float32)


def dot_nt(a, b):
    return lax.dot_general(a, b, (((1,), (1,)), ((), ())), preferred_element_type=jnp.float32)


def attn_kernel(q_ref, k_ref, v_ref, do_ref, cos_ref, sin_ref, bq_ref, bk_ref, bv_ref,
                o_ref, dlin_ref, gb_ref, qs, ks, vs, dkt, dvt):
    seq_len = q_ref.shape[0]
    start = pl.program_id(1) * HEAD_DIM
    third = dlin_ref.shape[1] // 3
    q_cols, k_cols, v_cols = (pl.ds(pl.multiple_of(start + j * third, HEAD_DIM), HEAD_DIM) for j in range(3))
    score_scale = HEAD_DIM ** -0.5
    cos_t = cos_ref[...]
    sin_t = sin_ref[...]
    half = HEAD_DIM // 2
    q_lin = q_ref[...] + bq_ref[...]
    qs[...] = (q_lin * cos_t + pltpu.roll(q_lin, half, 1) * sin_t).astype(jnp.bfloat16)
    k_lin = k_ref[...] + bk_ref[...]
    ks[...] = (k_lin * cos_t + pltpu.roll(k_lin, half, 1) * sin_t).astype(jnp.bfloat16)
    vs[...] = (v_ref[...] + bv_ref[...]).astype(jnp.bfloat16)
    row_i = lax.broadcasted_iota(jnp.int32, (BLOCK_Q, BLOCK_Q), 0)
    col_i = lax.broadcasted_iota(jnp.int32, (BLOCK_Q, BLOCK_Q), 1)
    causal = row_i >= col_i
    n_blocks = seq_len // BLOCK_Q
    gbq = jnp.zeros((1, HEAD_DIM), jnp.float32)
    for blk in reversed(range(n_blocks)):
        lo = blk * BLOCK_Q
        width = lo + BLOCK_Q
        q_b = qs[pl.ds(lo, BLOCK_Q), :]
        do_b = do_ref[pl.ds(lo, BLOCK_Q), :]
        k_all = ks[pl.ds(0, width), :]
        v_all = vs[pl.ds(0, width), :]
        scores = dot_nt(q_b, k_all) * score_scale
        tail = jnp.where(causal, scores[:, lo:], MASK_VALUE)
        scores = jnp.concatenate([scores[:, :lo], tail], axis=1) if lo else tail
        top = jnp.max(scores, axis=1, keepdims=True)
        prob = jnp.exp(scores - top)
        prob = prob * (1.0 / jnp.sum(prob, axis=1, keepdims=True))
        prob_b = prob.astype(jnp.bfloat16)
        o_ref[pl.ds(lo, BLOCK_Q), :] = dot_nn(prob_b, v_all).astype(jnp.bfloat16)
        d_prob = dot_nt(do_b, v_all)
        inner = jnp.sum(d_prob * prob, axis=1, keepdims=True)
        d_score = ((prob * (d_prob - inner)) * score_scale).astype(jnp.bfloat16)
        d_q = dot_nn(d_score, k_all)
        scaled = d_q * sin_ref[pl.ds(lo, BLOCK_Q), :]
        d_q = d_q * cos_ref[pl.ds(lo, BLOCK_Q), :] + pltpu.roll(scaled, half, 1)
        gbq = gbq + jnp.sum(d_q, axis=0, keepdims=True)
        dlin_ref[pl.ds(lo, BLOCK_Q), q_cols] = d_q.astype(jnp.bfloat16)
        dv_part = dot_nn(do_b.T, prob_b)
        dk_part = dot_nn(q_b.T, d_score)
        if blk == n_blocks - 1:
            dvt[...] = dv_part
            dkt[...] = dk_part
        else:
            dvt[:, pl.ds(0, width)] += dv_part
            dkt[:, pl.ds(0, width)] += dk_part
    d_v = dvt[...].T
    d_k = dkt[...].T
    d_k = d_k * cos_t + pltpu.roll(d_k * sin_t, half, 1)
    dlin_ref[:, v_cols] = d_v.astype(jnp.bfloat16)
    dlin_ref[:, k_cols] = d_k.astype(jnp.bfloat16)
    gb_ref[0, 0:1, q_cols] = gbq
    gb_ref[0, 0:1, k_cols] = jnp.sum(d_k, axis=0, keepdims=True)
    gb_ref[0, 0:1, v_cols] = jnp.sum(d_v, axis=0, keepdims=True)


def rope_tables(seq_len):
    half = HEAD_DIM // 2
    inv_freq = jnp.power(ROPE_THETA, -(jnp.arange(half, dtype=jnp.float32) * 2.0 / HEAD_DIM))
    angles = jnp.arange(seq_len, dtype=jnp.float32)[:, None] * inv_freq[None, :]
    cos_t = jnp.concatenate([jnp.cos(angles)] * 2, axis=-1)
    sin_t = jnp.concatenate([-jnp.sin(angles), jnp.sin(angles)], axis=-1)
    return cos_t, sin_t


def attention(lin, d_attn, bias, cos_t, sin_t):
    tokens, width = d_attn.shape
    seq_len = cos_t.shape[0]
    n_seq, n_heads = tokens // seq_len, width // HEAD_DIM
    tile = pl.BlockSpec((seq_len, HEAD_DIM), lambda s, h: (s, h))
    third = [pl.BlockSpec((seq_len, HEAD_DIM), lambda s, h, j=j: (s, j * n_heads + h)) for j in range(3)]
    third_b = [pl.BlockSpec((1, HEAD_DIM), lambda s, h, j=j: (0, j * n_heads + h)) for j in range(3)]
    table = pl.BlockSpec((seq_len, HEAD_DIM), lambda s, h: (0, 0))
    pairs = n_seq * n_heads * seq_len * seq_len
    head_buf = pltpu.VMEM((seq_len, HEAD_DIM), jnp.bfloat16)
    turned = pltpu.VMEM((HEAD_DIM, seq_len), jnp.float32)
    return pl.pallas_call(
        attn_kernel,
        grid=(n_seq, n_heads),
        in_specs=[*third, tile, table, table, *third_b],
        out_specs=[
            tile,
            pl.BlockSpec((seq_len, 3 * width), lambda s, h: (s, 0)),
            pl.BlockSpec((1, 8, 3 * width), lambda s, h: (s, 0, 0)),
        ],
        out_shape=[
            jax.ShapeDtypeStruct((tokens, width), jnp.bfloat16),
            jax.ShapeDtypeStruct((tokens, 3 * width), jnp.bfloat16),
            jax.ShapeDtypeStruct((n_seq, 8, 3 * width), jnp.float32),
        ],
        scratch_shapes=[head_buf, head_buf, head_buf, turned, turned],
        compiler_params=pltpu.CompilerParams(
            dimension_semantics=("arbitrary", "arbitrary"), vmem_limit_bytes=VMEM_MAX),
        cost_estimate=pl.CostEstimate(
            flops=6 * 2 * HEAD_DIM * pairs, bytes_accessed=22 * tokens * width, transcendentals=pairs),
        name="attn_fwd_bwd",
    )(lin, lin, lin, d_attn, cos_t, sin_t, bias, bias, bias)


def block_fwd_bwd(x_rows, hidden, inv_rms, grad_out, seq_len, gain_f, biases, w_groups, w_out, on_grad):
    f32 = jnp.float32
    tn = (((0,), (0,)), ((), ()))
    n_groups = len(w_groups)
    group = w_out.shape[0] // n_groups
    cos_t, sin_t = rope_tables(seq_len)
    x_full = x_rows.astype(f32)
    x_norm = x_full * inv_rms
    outs, d_lins, bias_grads, grad_ws = [], [], [], []
    hid = hidden
    for g in range(n_groups):
        lin = dot_nn(hid, w_groups[g])
        d_attn = dot_nt(grad_out, w_out[g * group:(g + 1) * group]).astype(jnp.bfloat16)
        o_g, d_lin, gb = attention(lin, d_attn, biases[g], cos_t, sin_t)
        grad_w = lax.dot_general(hidden, d_lin, tn, preferred_element_type=f32)
        hid, grad_w = lax.optimization_barrier((hidden, grad_w))
        grad_ws.append(on_grad(grad_w))
        outs.append(o_g)
        d_lins.append(d_lin)
        bias_grads.append(jnp.sum(gb[:, 0], axis=0))
    attn_b = jnp.concatenate(outs, axis=1)
    grad_wo = on_grad(lax.dot_general(attn_b, grad_out, tn, preferred_element_type=f32))
    block_out = (x_full + dot_nn(attn_b, w_out)).astype(jnp.bfloat16)
    d_hidden = dot_nt(d_lins[0], w_groups[0])
    for g in range(1, n_groups):
        d_hidden = d_hidden + dot_nt(d_lins[g], w_groups[g])
    grad_gain = jnp.sum(d_hidden * x_norm, axis=0)
    d_norm = d_hidden * gain_f
    d_x = grad_out.astype(f32) + inv_rms * (d_norm - x_norm * jnp.mean(d_norm * x_norm, axis=-1, keepdims=True))
    return block_out, d_x, grad_ws, grad_wo, grad_gain, jnp.stack(bias_grads)


def barrier_all(me):
    barrier = pltpu.get_barrier_semaphore()
    for step in range(1, N_DEV):
        pl.semaphore_signal(barrier, inc=1, device_id=(jnp.bitwise_xor(me, step),), device_id_type=MESH)
    pl.semaphore_wait(barrier, N_DEV - 1)


LOOK_CHUNK = 128
LOOK_N = HOT // 2 // LOOK_CHUNK


def lookup_kernel(cold_ref, _, vec_ref, rows_ref, got_ref, vgot_ref,
                  recv_sem, link_sem, mate_sem, c_send, c_recv, v_send, v_recv, l_sem):
    me = lax.axis_index(AXIS)
    chip, core = me // 2, me % 2
    barrier_all(me)
    own = pltpu.make_async_copy(cold_ref.at[me], got_ref.at[me], l_sem.at[0])
    own_v = pltpu.make_async_copy(vec_ref, vgot_ref.at[me], l_sem.at[1])
    own.start()
    own_v.start()

    def cold_copy(step):
        peer = jnp.bitwise_xor(me, step)
        return pltpu.make_async_remote_copy(
            src_ref=cold_ref.at[peer], dst_ref=got_ref.at[me],
            send_sem=c_send.at[step - 1], recv_sem=c_recv.at[step - 1],
            device_id=(peer,), device_id_type=MESH)

    def vec_copy(step):
        peer = jnp.bitwise_xor(me, step)
        return pltpu.make_async_remote_copy(
            src_ref=vec_ref, dst_ref=vgot_ref.at[me], send_sem=v_send.at[step - 1], recv_sem=v_recv.at[step - 1],
            device_id=(peer,), device_id_type=MESH)

    def piece(part, k):
        return rows_ref.at[pl.ds(part * (HOT // 2) + k * LOOK_CHUNK, LOOK_CHUNK)]

    def link_copy(part, k, target):
        return pltpu.make_async_remote_copy(
            src_ref=piece(part, k), dst_ref=piece(part, k), send_sem=link_sem.at[part, k],
            recv_sem=recv_sem.at[part, k], device_id=(target,), device_id_type=MESH)

    def mate_copy(part, k):
        return pltpu.make_async_remote_copy(
            src_ref=piece(part, k), dst_ref=piece(part, k), send_sem=mate_sem.at[part, k],
            recv_sem=recv_sem.at[part, k], device_id=(jnp.bitwise_xor(me, 1),), device_id_type=MESH)

    place = [
        jnp.where(chip == 0, 0, jnp.where(chip == 1, 1, jnp.where(chip == 3, 2, 3))),
        jnp.where(chip == 0, 0, jnp.where(chip == 2, 1, jnp.where(chip == 3, 2, 3))),
    ]
    target = [
        2 * jnp.where(chip == 0, 1, jnp.where(chip == 1, 3, 2)),
        2 * jnp.where(chip == 0, 2, jnp.where(chip == 2, 3, 1)),
    ]

    def stage(step, carry):
        for part in range(2):
            k = step - place[part]
            live = (k >= 0) & (k < LOOK_N)

            @pl.when(live & (me != 0))
            def _():
                mate_copy(part, k).wait_recv()

            @pl.when(live & (core == 0) & (place[part] < 3))
            def _():
                link_copy(part, k, target[part]).start()

            @pl.when(live & (core == 0))
            def _():
                mate_copy(part, k).start()
        return carry

    for step in range(1, N_DEV):
        vec_copy(step).start()
        cold_copy(step).start()
    lax.fori_loop(0, LOOK_N + 3, stage, 0)

    def drain(k, carry):
        for part in range(2):
            @pl.when((core == 0) & (place[part] < 3))
            def _():
                link_copy(part, k, target[part]).wait_send()

            @pl.when(core == 0)
            def _():
                mate_copy(part, k).wait_send()
        return carry

    lax.fori_loop(0, LOOK_N, drain, 0)
    for step in range(1, N_DEV):
        vec_copy(step).wait()
        cold_copy(step).wait()
    own.wait()
    own_v.wait()


def lookup_exchange(cold_send, hot_rows, vecs):
    any_spec = pl.BlockSpec(memory_space=pl.ANY)
    dma = pltpu.SemaphoreType.DMA
    return pl.pallas_call(
        lookup_kernel,
        out_shape=[
            jax.ShapeDtypeStruct(hot_rows.shape, hot_rows.dtype),
            jax.ShapeDtypeStruct(cold_send.shape, cold_send.dtype),
            jax.ShapeDtypeStruct((N_DEV,) + vecs.shape, vecs.dtype),
        ],
        in_specs=[any_spec] * 3,
        out_specs=[any_spec] * 3,
        scratch_shapes=[dma((2, LOOK_N))] * 3 + [dma((N_DEV - 1,))] * 4 + [dma((2,))],
        input_output_aliases={1: 0},
        compiler_params=pltpu.CompilerParams(collective_id=0, has_side_effects=True),
        name="lookup_exchange",
    )(cold_send, hot_rows, vecs)


def pick_kernel(idx_ref, hot_ref, cold_ref, gain_ref, x_ref, hid_ref, inv_ref, rows, picked, sem):
    step = pl.program_id(0)
    count, width = x_ref.shape
    base = step * count

    @pl.when(step == 0)
    def _():
        hot = pltpu.make_async_copy(hot_ref, rows.at[pl.ds(0, HOT)], sem.at[0])
        cold = pltpu.make_async_copy(cold_ref, rows.at[pl.ds(HOT, cold_ref.shape[0])], sem.at[1])
        hot.start()
        cold.start()
        hot.wait()
        cold.wait()

    def body(i8, carry):
        for j in range(8):
            i = i8 * 8 + j
            picked[i] = rows[idx_ref[base + i]]
        return carry

    lax.fori_loop(0, count // 8, body, 0)
    x = picked[...].reshape(count, width)
    x_ref[...] = x
    x_full = x.astype(jnp.float32)
    inv = lax.rsqrt(jnp.mean(x_full * x_full, axis=-1, keepdims=True) + NORM_EPS)
    inv_ref[...] = inv
    hid_ref[...] = (x_full * inv * gain_ref[...]).astype(jnp.bfloat16)


def pick_rows(idx, hot, cold, gain, block):
    count = idx.shape[0]
    tail = hot.shape[1:]
    width = tail[0] * tail[1]
    any_spec = pl.BlockSpec(memory_space=pl.ANY)
    wide = pl.BlockSpec((block, width), lambda i, s: (i, 0))
    act = jax.ShapeDtypeStruct((count, width), hot.dtype)
    return pl.pallas_call(
        pick_kernel,
        grid_spec=pltpu.PrefetchScalarGridSpec(
            num_scalar_prefetch=1,
            grid=(count // block,),
            in_specs=[any_spec, any_spec, pl.BlockSpec((1, width), lambda i, s: (0, 0))],
            out_specs=[wide, wide, pl.BlockSpec((block, 1), lambda i, s: (i, 0))],
            scratch_shapes=[
                pltpu.VMEM((hot.shape[0] + cold.shape[0],) + tail, hot.dtype),
                pltpu.VMEM((block,) + tail, hot.dtype),
                pltpu.SemaphoreType.DMA((2,)),
            ],
        ),
        out_shape=[act, act, jax.ShapeDtypeStruct((count, 1), jnp.float32)],
        compiler_params=pltpu.CompilerParams(dimension_semantics=("arbitrary",), vmem_limit_bytes=VMEM_MAX),
        name="pick_rows",
    )(idx, hot, cold, gain)


def take2d_kernel(idx_ref, idx2_ref, rows_ref, out_ref, out2_ref, buf):
    step = pl.program_id(0)

    def copy_rows(idx, dst, count):
        def body(i8, carry):
            for j in range(8):
                i = i8 * 8 + j
                dst[pl.ds(i, 1), :] = rows_ref[pl.ds(idx[step * count + i], 1), :]
            return carry

        lax.fori_loop(0, count // 8, body, 0)

    copy_rows(idx_ref, buf, buf.shape[0])
    out_ref[...] = buf[...].astype(out_ref.dtype)
    copy_rows(idx2_ref, out2_ref, out2_ref.shape[0])


def take2d(idx, idx2, rows, steps):
    count, count2 = idx.shape[0] // steps, idx2.shape[0] // steps
    width = rows.shape[1]
    return pl.pallas_call(
        take2d_kernel,
        grid_spec=pltpu.PrefetchScalarGridSpec(
            num_scalar_prefetch=2,
            grid=(steps,),
            in_specs=[pl.BlockSpec(rows.shape, lambda i, a, b: (0, 0), pipeline_mode=pl.Buffered(1))],
            out_specs=[
                pl.BlockSpec((count, width), lambda i, a, b: (i, 0)),
                pl.BlockSpec((count2, width), lambda i, a, b: (i, 0)),
            ],
            scratch_shapes=[pltpu.VMEM((count, width), jnp.float32)],
        ),
        out_shape=[
            jax.ShapeDtypeStruct((count * steps, width), jnp.bfloat16),
            jax.ShapeDtypeStruct((count2 * steps, width), jnp.float32),
        ],
        compiler_params=pltpu.CompilerParams(dimension_semantics=("arbitrary",), vmem_limit_bytes=VMEM_MAX),
        name="take_rows",
    )(idx, idx2, rows)


def seg_sum_kernel(key_ref, off_ref, mine_ref, mate_ref, out_ref, src, sem):
    blk = pl.program_id(0)
    count = mine_ref.shape[0]

    @pl.when(blk == 0)
    def _():
        first = pltpu.make_async_copy(mine_ref, src.at[pl.ds(0, count)], sem.at[0])
        second = pltpu.make_async_copy(mate_ref, src.at[pl.ds(count, count)], sem.at[1])
        first.start()
        second.start()
        first.wait()
        second.wait()

    out_ref[...] = jnp.zeros_like(out_ref)

    def body(e, carry):
        key = key_ref[e]
        row = lax.shift_right_logical(key, 12) - blk * ROW_BLOCK
        tok = jnp.bitwise_and(key, 4095)
        out_ref[pl.ds(row, 1), :] += src[pl.ds(tok, 1), :]
        return carry

    lax.fori_loop(off_ref[blk], off_ref[blk + 1], body, 0)


def seg_sum(keys, offs, dx_mine, dx_mate, n_rows):
    tokens, width = dx_mine.shape
    any_spec = pl.BlockSpec(memory_space=pl.ANY)
    return pl.pallas_call(
        seg_sum_kernel,
        grid_spec=pltpu.PrefetchScalarGridSpec(
            num_scalar_prefetch=2,
            grid=(n_rows // ROW_BLOCK,),
            in_specs=[any_spec, any_spec],
            out_specs=pl.BlockSpec((ROW_BLOCK, width), lambda i, a, b: (i, 0)),
            scratch_shapes=[pltpu.VMEM((2 * tokens, width), jnp.float32), pltpu.SemaphoreType.DMA((2,))],
        ),
        out_shape=jax.ShapeDtypeStruct((n_rows, width), jnp.float32),
        compiler_params=pltpu.CompilerParams(dimension_semantics=("arbitrary",), vmem_limit_bytes=VMEM_MAX),
        name="hot_seg_sum",
    )(keys, offs, dx_mine, dx_mate)


RED_CHUNK = 64
RED_N = HOT // 2 // RED_CHUNK


def reduce_kernel(part_ref, cold_ref, more_ref, vec_ref, hot_ref, crecv_ref, mrecv_ref, vrecv_ref,
                  local, incoming, load_sem, send_sem, recv_sem, out_sem,
                  c_send, c_recv, m_send, m_recv, v_send, v_recv, l_sem):
    me = lax.axis_index(AXIS)
    chip, core = me // 2, me % 2
    mid = jnp.where(core == 0, 1, 2)
    first = 3 - mid
    place = jnp.where(chip == first, 0, jnp.where(chip == 3, 1, jnp.where(chip == mid, 2, 3)))
    nxt = jnp.where(chip == first, 3, jnp.where(chip == 3, mid, 0))
    target = nxt * 2 + core

    def rows(k):
        return pl.ds(k * RED_CHUNK, RED_CHUNK)

    def load(k):
        return pltpu.make_async_copy(part_ref.at[rows(k)], local.at[rows(k)], load_sem.at[k])

    def send(k):
        return pltpu.make_async_remote_copy(
            src_ref=local.at[rows(k)], dst_ref=incoming.at[rows(k)], send_sem=send_sem.at[k],
            recv_sem=recv_sem.at[k], device_id=(target,), device_id_type=MESH)

    def put_own(k):
        return pltpu.make_async_copy(local.at[rows(k)], hot_ref.at[rows(k)], send_sem.at[k])

    def put_far(k):
        return pltpu.make_async_remote_copy(
            src_ref=local.at[rows(k)], dst_ref=hot_ref.at[pl.ds(HOT // 2 + k * RED_CHUNK, RED_CHUNK)],
            send_sem=send_sem.at[k], recv_sem=out_sem.at[k], device_id=(jnp.bitwise_xor(me, 1),), device_id_type=MESH)

    swaps = (
        (vec_ref, vrecv_ref, v_send, v_recv),
        (more_ref, mrecv_ref, m_send, m_recv),
        (cold_ref, crecv_ref, c_send, c_recv),
    )

    def swap(which, step):
        src, dst, s_sem, r_sem = swaps[which]
        peer = jnp.bitwise_xor(me, step)
        return pltpu.make_async_remote_copy(
            src_ref=src.at[peer], dst_ref=dst.at[me], send_sem=s_sem.at[step - 1], recv_sem=r_sem.at[step - 1],
            device_id=(peer,), device_id_type=MESH)

    def keep(which):
        src, dst, _, _ = swaps[which]
        return pltpu.make_async_copy(src.at[me], dst.at[me], l_sem.at[which])

    def start_load(k, carry):
        load(k).start()
        return carry

    lax.fori_loop(0, RED_N, start_load, 0)
    barrier_all(me)
    for which in range(3):
        keep(which).start()
    for which in range(3):
        for step in range(1, N_DEV):
            swap(which, step).start()

    def stage(k, carry):
        @pl.when(k < RED_N)
        def _():
            load(k).wait()

        @pl.when((k < RED_N) & (place > 0))
        def _():
            send(k).wait_recv()
            local[rows(k), :] += incoming[rows(k), :]

        @pl.when((k >= 1) & (place < 3))
        def _():
            send(k - 1).start()

        @pl.when((k >= 1) & (me == 0))
        def _():
            put_own(k - 1).start()

        @pl.when((k >= 1) & (me == 1))
        def _():
            put_far(k - 1).start()
        return carry

    lax.fori_loop(0, RED_N + 1, stage, 0)

    def drain(k, carry):
        @pl.when(place < 3)
        def _():
            send(k).wait_send()

        @pl.when(me == 0)
        def _():
            put_own(k).wait()
            put_far(k).wait_recv()

        @pl.when(me == 1)
        def _():
            put_far(k).wait_send()
        return carry

    lax.fori_loop(0, RED_N, drain, 0)
    for which in range(3):
        for step in range(1, N_DEV):
            swap(which, step).wait()
        keep(which).wait()


def grad_exchange(part, cold_send, more_send, vecs):
    any_spec = pl.BlockSpec(memory_space=pl.ANY)
    dma = pltpu.SemaphoreType.DMA
    width = part.shape[1]
    return pl.pallas_call(
        reduce_kernel,
        out_shape=[jax.ShapeDtypeStruct((HOT, width), jnp.float32)]
        + [jax.ShapeDtypeStruct(a.shape, a.dtype) for a in (cold_send, more_send, vecs)],
        in_specs=[any_spec] * 4,
        out_specs=[any_spec] * 4,
        scratch_shapes=[pltpu.VMEM(part.shape, jnp.float32)] * 2
        + [dma((RED_N,))] * 4 + [dma((N_DEV - 1,))] * 6 + [dma((3,))],
        compiler_params=pltpu.CompilerParams(
            collective_id=1, has_side_effects=True, vmem_limit_bytes=VMEM_MAX),
        name="grad_exchange",
    )(part, cold_send, more_send, vecs)


def table_kernel(key_ref, off_ref, n_hot_ref, src_ref, more_ref, hot_ref, out_ref, acc, rows, half_rows, sem):
    blk = pl.program_id(0)
    n_src = src_ref.shape[0]

    @pl.when(blk == 0)
    def _():
        low = pltpu.make_async_copy(src_ref, half_rows, sem.at[0])
        high = pltpu.make_async_copy(more_ref, rows.at[pl.ds(n_src, more_ref.shape[0])], sem.at[1])
        low.start()
        high.start()
        low.wait()
        for c in range(N_DEV):
            part = pl.ds(c * (n_src // N_DEV), n_src // N_DEV)
            rows[part, :] = half_rows[part, :].astype(jnp.float32)
        high.wait()

    is_hot = blk < n_hot_ref[0]

    @pl.when(is_hot)
    def _():
        acc[...] = hot_ref[...]

    @pl.when(jnp.logical_not(is_hot))
    def _():
        acc[...] = jnp.zeros_like(acc)

    def body(e, carry):
        key = key_ref[e]
        row = lax.shift_right_logical(key, 11) - blk * ROW_BLOCK
        idx = jnp.bitwise_and(key, 2047)
        acc[pl.ds(row, 1), :] += rows[pl.ds(idx, 1), :]
        return carry

    lax.fori_loop(off_ref[blk], off_ref[blk + 1], body, 0)
    out_ref[...] = acc[...].astype(out_ref.dtype)


def build_table(keys, offs, n_hot, src, more, hot, n_rows):
    width = src.shape[1]

    def hot_index(i, k, o, n):
        return (jnp.minimum(i, jnp.maximum(n[0] - 1, 0)), 0)

    return pl.pallas_call(
        table_kernel,
        grid_spec=pltpu.PrefetchScalarGridSpec(
            num_scalar_prefetch=3,
            grid=(pl.cdiv(n_rows, ROW_BLOCK),),
            in_specs=[
                pl.BlockSpec(memory_space=pl.ANY),
                pl.BlockSpec(memory_space=pl.ANY),
                pl.BlockSpec((ROW_BLOCK, width), hot_index),
            ],
            out_specs=pl.BlockSpec((ROW_BLOCK, width), lambda i, k, o, n: (i, 0)),
            scratch_shapes=[
                pltpu.VMEM((ROW_BLOCK, width), jnp.float32),
                pltpu.VMEM((src.shape[0] + more.shape[0], width), jnp.float32),
                pltpu.VMEM(src.shape, src.dtype),
                pltpu.SemaphoreType.DMA((2,)),
            ],
        ),
        out_shape=jax.ShapeDtypeStruct((n_rows, width), jnp.bfloat16),
        compiler_params=pltpu.CompilerParams(dimension_semantics=("arbitrary",), vmem_limit_bytes=VMEM_MAX),
        name="build_table",
    )(keys, offs, n_hot, src, more, hot)


def fast_lookup(all_ids, own_ids, table_part, gain_vecs, me):
    rows_dev, width = table_part.shape
    tokens = own_ids.shape[0]
    first_row = me * rows_dev
    t_idx = jnp.arange(tokens, dtype=jnp.int32)
    mine = (all_ids >= HOT) & (all_ids >= first_row) & (all_ids < first_row + rows_dev)
    key = jnp.where(mine, t_idx[None, :] * 32768 + (all_ids - first_row), BIG)
    key = lax.sort(key, dimension=1)[:, :CAP]
    asked = key != BIG
    ask_row = jnp.where(asked, jnp.bitwise_and(key, 32767), 0)
    send = jnp.take(table_part, ask_row.reshape(-1), axis=0, mode="clip")
    tiles = (width // LANES, LANES)
    send = send.reshape((N_DEV, CAP) + tiles)
    hot, cold, vecs = lookup_exchange(send, table_part[:HOT].reshape((HOT,) + tiles), gain_vecs)
    vecs = vecs.transpose(1, 0, 2).reshape(gain_vecs.shape[0], -1).astype(jnp.float32)
    owners = own_ids // rows_dev
    hit = (owners[None, :] == jnp.arange(N_DEV, dtype=jnp.int32)[:, None]) & (own_ids >= HOT)[None, :]
    place = jnp.cumsum(hit.astype(jnp.int32), axis=1) - 1 + jnp.arange(N_DEV, dtype=jnp.int32)[:, None] * CAP
    slot = jnp.sum(jnp.where(hit, place, 0), axis=0)
    idx = jnp.where(own_ids >= HOT, HOT + slot, own_ids)
    normed = pick_rows(idx, hot, cold.reshape((N_DEV * CAP,) + tiles), vecs[:1], 256)
    return normed, cold, vecs


def first_of(mask, values, count):
    return lax.sort(jnp.where(mask, values, BIG), dimension=1)[:, :count]


def grad_plan(all_ids, own_ids, me, rows_dev):
    tokens = own_ids.shape[0]
    flat = all_ids.reshape(-1).astype(jnp.uint32)
    pos = jnp.arange(flat.shape[0], dtype=jnp.uint32)
    ordered = lax.sort(flat * jnp.uint32(16384) + pos)
    ident = ordered // jnp.uint32(16384)
    same = ident[1:] == ident[:-1]
    no = jnp.zeros((1,), jnp.bool_)
    again = jnp.concatenate([no, same]) | jnp.concatenate([same, no])
    again = lax.sort((ordered % jnp.uint32(16384)) * jnp.uint32(2) + again.astype(jnp.uint32)) % jnp.uint32(2)
    again = (again == 1).reshape(all_ids.shape)
    t_idx = jnp.arange(tokens, dtype=jnp.int32)[None, :]
    devices = jnp.arange(N_DEV, dtype=jnp.int32)
    owners = jnp.where(all_ids >= HOT, all_ids // rows_dev, -1)
    counts = jnp.sum(((owners[None] == devices[:, None, None]) & again[None]).astype(jnp.int32), axis=-1)
    fits = jnp.max(counts) <= MORE
    hit = lax.dynamic_index_in_dim(owners, me, 0, keepdims=False)[None, :] == devices[:, None]
    own_again = lax.dynamic_index_in_dim(again, me, 0, keepdims=True)
    slot_tok = first_of(hit, t_idx, CAP)
    more_tok = first_of(hit & own_again, t_idx, MORE)
    mine = owners == me
    local = all_ids - me * rows_dev
    row = first_of(mine, t_idx * 65536 + local * 2 + again, CAP)
    more_row = first_of(mine & again, t_idx * 65536 + local * 2 + again, MORE)
    slots = jnp.arange(N_DEV * CAP, dtype=jnp.int32).reshape(N_DEV, CAP)
    more_slots = N_DEV * CAP + jnp.arange(N_DEV * MORE, dtype=jnp.int32).reshape(N_DEV, MORE)

    def owner_key(packed, slot, wanted):
        where = jnp.bitwise_and(lax.shift_right_logical(packed, 1), 32767)
        return jnp.where((packed != BIG) & (jnp.bitwise_and(packed, 1) == wanted), where * 2048 + slot, BIG).reshape(-1)

    owner_keys = lax.sort(jnp.concatenate([owner_key(row, slots, 0), owner_key(more_row, more_slots, 1)]))

    def clean(tok):
        return jnp.where(tok == BIG, 0, tok).reshape(-1)

    return fits, clean(slot_tok), clean(more_tok), owner_keys


def block_offsets(keys, n_blocks, shift):
    edges = jnp.arange(n_blocks + 1, dtype=jnp.int32) * (ROW_BLOCK << shift)
    return jnp.sum(keys[None, :] < edges[:, None], axis=1).astype(jnp.int32)


def fast_table_grad(rows_dev, all_ids, own_ids, d_x, vecs, slot_tok, more_tok, owner_keys):
    tokens, width = d_x.shape
    me = lax.axis_index(AXIS)
    mate_of = [(i, i ^ 1) for i in range(N_DEV)]
    dx_mate = lax.ppermute(d_x, AXIS, mate_of)
    mate_ids = lax.dynamic_index_in_dim(all_ids, jnp.bitwise_xor(me, 1), 0, keepdims=False)
    pair_ids = jnp.concatenate([own_ids, mate_ids])
    base = (me % 2) * (HOT // 2)
    inside = (pair_ids >= base) & (pair_ids < base + HOT // 2)
    keys = jnp.where(inside, (pair_ids - base) * 4096 + jnp.arange(2 * tokens, dtype=jnp.int32), BIG)
    keys = lax.sort(keys)
    part = seg_sum(keys, block_offsets(keys, HOT // 2 // ROW_BLOCK, 12), d_x, dx_mate, HOT // 2)
    cold, more = take2d(slot_tok, more_tok, d_x, N_DEV)
    cold = cold.reshape(N_DEV, CAP, width)
    more = more.reshape(N_DEV, MORE, width)
    hot, recv, more_recv, vec_recv = grad_exchange(part, cold, more, vecs)
    n_hot = jnp.where(me == 0, HOT // ROW_BLOCK, 0).astype(jnp.int32)[None]
    offs = block_offsets(owner_keys, pl.cdiv(rows_dev, ROW_BLOCK), 11)
    recv = recv.reshape(N_DEV * CAP, width)
    more_recv = more_recv.reshape(N_DEV * MORE, width)
    grad_part = build_table(owner_keys, offs, n_hot, recv, more_recv, hot, rows_dev)
    return grad_part, jnp.sum(vec_recv, axis=0)


def slow_lookup(all_ids, table_part, me):
    rows_dev = table_part.shape[0]
    local_idx = all_ids - me * rows_dev
    is_owned = (local_idx >= 0) & (local_idx < rows_dev)
    looked = jnp.take(table_part, jnp.where(is_owned, local_idx, 0), axis=0)
    looked = jnp.where(is_owned[..., None], looked, jnp.zeros((), jnp.bfloat16))
    return lax.psum_scatter(looked, AXIS, scatter_dimension=0)


def slow_table_grad(rows_dev, all_ids, own_ids, d_x, vecs, *_):
    me = lax.axis_index(AXIS)
    local_idx = all_ids - me * rows_dev
    is_owned = (local_idx >= 0) & (local_idx < rows_dev)
    all_dx = lax.all_gather(d_x, AXIS)
    seg_idx = jnp.where(is_owned, local_idx, rows_dev)
    grad_part = jax.ops.segment_sum(all_dx.reshape(-1, d_x.shape[-1]), seg_idx.reshape(-1), num_segments=rows_dev)
    return grad_part.astype(jnp.bfloat16), lax.psum_scatter(vecs, AXIS, scatter_dimension=0)


def solution(mesh):
    row_spec = P(AXIS, None)
    vec_spec = P(AXIS)
    act_spec = P(AXIS, None, None)
    weight_specs = (vec_spec, row_spec, vec_spec, row_spec, vec_spec, row_spec, vec_spec, row_spec)
    in_specs = (row_spec, act_spec, row_spec) + weight_specs
    out_specs = (act_spec, row_spec) + weight_specs

    def run(fast, tok_ids, all_ids, grad_out, table_part, gain_part, wq_part, bq_part, wk_part, bk_part, wv_part, bv_part, wo_part):
        me = lax.axis_index(AXIS)
        rows_dev, width = table_part.shape
        n_seq, seq_len = tok_ids.shape
        own_ids = tok_ids.reshape(-1)

        def whole(part):
            return lax.all_gather(part, AXIS, axis=0, tiled=True)

        def scatter(grad):
            return lax.psum_scatter(grad, AXIS, scatter_dimension=0, tiled=True)

        part_w = gain_part.shape[0]
        group = wq_part.shape[1] // GROUPS
        cols = [slice(g * group, (g + 1) * group) for g in range(GROUPS)]
        vec_parts = jnp.pad(jnp.stack([gain_part, bq_part, bk_part, bv_part]), ((0, 12), (0, 0)))
        w_parts = [jnp.concatenate([wq_part[:, c], wk_part[:, c], wv_part[:, c]], axis=1) for c in cols]
        if fast:
            (x_rows, hidden, inv_rms), marker, vec_full = fast_lookup(all_ids, own_ids, table_part, vec_parts, me)
            late = lax.optimization_barrier((marker, *w_parts[1:]))
            w_parts = [w_parts[0], *late[1:]]
        else:
            x_rows = slow_lookup(all_ids, table_part, me)
            vec_full = lax.all_gather(vec_parts, AXIS, axis=1, tiled=True).astype(jnp.float32)
            x_full = x_rows.astype(jnp.float32)
            inv_rms = lax.rsqrt(jnp.mean(x_full * x_full, axis=-1, keepdims=True) + NORM_EPS)
            hidden = (x_full * inv_rms * vec_full[0]).astype(jnp.bfloat16)
        biases = [jnp.concatenate([vec_full[1, c], vec_full[2, c], vec_full[3, c]])[None] for c in cols]
        wo_full = whole(wo_part)
        w_groups = [whole(part) for part in w_parts]
        grad_flat = grad_out.reshape(-1, width)
        block_out, d_x, grad_ws, grad_wo, grad_gain, grad_bias = block_fwd_bwd(
            x_rows, hidden, inv_rms, grad_flat, seq_len, vec_full[0], biases, w_groups, wo_full, scatter)
        gq, gk, gv = (
            jnp.concatenate([grad_w[:, j * group:(j + 1) * group] for grad_w in grad_ws], axis=1) for j in range(3))
        grad_bias = grad_bias.reshape(GROUPS, 3, group)
        vecs = jnp.stack([grad_gain] + [grad_bias[:, j].reshape(-1) for j in range(3)])
        vecs = jnp.pad(vecs.reshape(4, N_DEV, part_w).transpose(1, 0, 2), ((0, 0), (0, 4), (0, 0)))
        rest = (all_ids, own_ids, d_x, vecs)
        if fast:
            few, slot_tok, more_tok, owner_keys = grad_plan(all_ids, own_ids, me, rows_dev)
            rest = rest + (slot_tok, more_tok, owner_keys)
            grad_part, vec_sum = lax.cond(
                few, functools.partial(fast_table_grad, rows_dev), functools.partial(slow_table_grad, rows_dev), *rest)
        else:
            grad_part, vec_sum = slow_table_grad(rows_dev, *rest)
        return (block_out.reshape(grad_out.shape), grad_part, vec_sum[0], gq, vec_sum[1], gk, vec_sum[2], gv, vec_sum[3], grad_wo)

    def device_step(tok_ids, grad_out, table_part, *weights):
        rows_dev = table_part.shape[0]
        all_ids = lax.all_gather(tok_ids.reshape(-1), AXIS)
        owners = jnp.where(all_ids >= HOT, all_ids // rows_dev, -1)
        counts = jnp.sum((owners[None] == jnp.arange(N_DEV, dtype=jnp.int32)[:, None, None]).astype(jnp.int32), axis=-1)
        fits = jnp.max(counts) <= CAP
        args = (tok_ids, all_ids, grad_out, table_part) + weights
        return lax.cond(fits, functools.partial(run, True), functools.partial(run, False), *args)

    return jax.shard_map(device_step, mesh=mesh, in_specs=in_specs, out_specs=out_specs, check_vma=False)
```

```python
import functools

import jax
import jax.numpy as jnp
from jax import lax
from jax.experimental import pallas as pl
from jax.experimental.pallas import tpu as pltpu
from jax.sharding import PartitionSpec as P

HEAD_DIM = 128
ROPE_THETA = 1.0e6
NORM_EPS = 1e-6
MASK_VALUE = -1e30
AXIS = "fsdp"
N_DEV = 8
HOT = 4096
CAP = 176
MORE = 24
LANES = 128
BIG = 2**31 - 1
MESH = pl.DeviceIdType.MESH
BLOCK_Q = 512
GROUPS = 4
ROW_BLOCK = 128
TABLE_BLOCK = 512
VMEM_MAX = 60 * 1024 * 1024


def dot_nn(a, b):
    return lax.dot_general(a, b, (((1,), (0,)), ((), ())), preferred_element_type=jnp.float32)


def dot_nt(a, b):
    return lax.dot_general(a, b, (((1,), (1,)), ((), ())), preferred_element_type=jnp.float32)


def attn_kernel(q_ref, k_ref, v_ref, do_ref, cos_ref, sin_ref, bq_ref, bk_ref, bv_ref,
                o_ref, dlin_ref, gb_ref, qs, ks, vs, dkt, dvt):
    seq_len = q_ref.shape[0]
    start = pl.program_id(1) * HEAD_DIM
    third = dlin_ref.shape[1] // 3
    q_cols, k_cols, v_cols = (pl.ds(pl.multiple_of(start + j * third, HEAD_DIM), HEAD_DIM) for j in range(3))
    score_scale = HEAD_DIM ** -0.5
    cos_t = cos_ref[...]
    sin_t = sin_ref[...]
    half = HEAD_DIM // 2
    q_lin = q_ref[...] + bq_ref[...]
    qs[...] = (q_lin * cos_t + pltpu.roll(q_lin, half, 1) * sin_t).astype(jnp.bfloat16)
    k_lin = k_ref[...] + bk_ref[...]
    ks[...] = (k_lin * cos_t + pltpu.roll(k_lin, half, 1) * sin_t).astype(jnp.bfloat16)
    vs[...] = (v_ref[...] + bv_ref[...]).astype(jnp.bfloat16)
    row_i = lax.broadcasted_iota(jnp.int32, (BLOCK_Q, BLOCK_Q), 0)
    col_i = lax.broadcasted_iota(jnp.int32, (BLOCK_Q, BLOCK_Q), 1)
    causal = row_i >= col_i
    n_blocks = seq_len // BLOCK_Q
    gbq = jnp.zeros((1, HEAD_DIM), jnp.float32)
    for blk in reversed(range(n_blocks)):
        lo = blk * BLOCK_Q
        width = lo + BLOCK_Q
        q_b = qs[pl.ds(lo, BLOCK_Q), :]
        do_b = do_ref[pl.ds(lo, BLOCK_Q), :]
        k_all = ks[pl.ds(0, width), :]
        v_all = vs[pl.ds(0, width), :]
        scores = dot_nt(q_b, k_all) * score_scale
        tail = jnp.where(causal, scores[:, lo:], MASK_VALUE)
        scores = jnp.concatenate([scores[:, :lo], tail], axis=1) if lo else tail
        top = jnp.max(scores, axis=1, keepdims=True)
        prob = jnp.exp(scores - top)
        prob = prob * (1.0 / jnp.sum(prob, axis=1, keepdims=True))
        prob_b = prob.astype(jnp.bfloat16)
        o_ref[pl.ds(lo, BLOCK_Q), :] = dot_nn(prob_b, v_all).astype(jnp.bfloat16)
        d_prob = dot_nt(do_b, v_all)
        inner = jnp.sum(d_prob * prob, axis=1, keepdims=True)
        d_score = ((prob * (d_prob - inner)) * score_scale).astype(jnp.bfloat16)
        d_q = dot_nn(d_score, k_all)
        scaled = d_q * sin_ref[pl.ds(lo, BLOCK_Q), :]
        d_q = d_q * cos_ref[pl.ds(lo, BLOCK_Q), :] + pltpu.roll(scaled, half, 1)
        gbq = gbq + jnp.sum(d_q, axis=0, keepdims=True)
        dlin_ref[pl.ds(lo, BLOCK_Q), q_cols] = d_q.astype(jnp.bfloat16)
        dv_part = dot_nn(do_b.T, prob_b)
        dk_part = dot_nn(q_b.T, d_score)
        if blk == n_blocks - 1:
            dvt[...] = dv_part
            dkt[...] = dk_part
        else:
            dvt[:, pl.ds(0, width)] += dv_part
            dkt[:, pl.ds(0, width)] += dk_part
    d_v = dvt[...].T
    d_k = dkt[...].T
    d_k = d_k * cos_t + pltpu.roll(d_k * sin_t, half, 1)
    dlin_ref[:, v_cols] = d_v.astype(jnp.bfloat16)
    dlin_ref[:, k_cols] = d_k.astype(jnp.bfloat16)
    gb_ref[0, 0:1, q_cols] = gbq
    gb_ref[0, 0:1, k_cols] = jnp.sum(d_k, axis=0, keepdims=True)
    gb_ref[0, 0:1, v_cols] = jnp.sum(d_v, axis=0, keepdims=True)


def rope_tables(seq_len):
    half = HEAD_DIM // 2
    inv_freq = jnp.power(ROPE_THETA, -(jnp.arange(half, dtype=jnp.float32) * 2.0 / HEAD_DIM))
    angles = jnp.arange(seq_len, dtype=jnp.float32)[:, None] * inv_freq[None, :]
    cos_t = jnp.concatenate([jnp.cos(angles)] * 2, axis=-1)
    sin_t = jnp.concatenate([-jnp.sin(angles), jnp.sin(angles)], axis=-1)
    return cos_t, sin_t


def attention(lin, d_attn, bias, cos_t, sin_t, part, parts):
    tokens = lin.shape[0]
    width = d_attn.shape[1] // parts
    seq_len = cos_t.shape[0]
    n_seq, n_heads = tokens // seq_len, width // HEAD_DIM
    tile = pl.BlockSpec((seq_len, HEAD_DIM), lambda s, h: (s, h))
    third = [pl.BlockSpec((seq_len, HEAD_DIM), lambda s, h, j=j: (s, j * n_heads + h)) for j in range(3)]
    third_b = [pl.BlockSpec((1, HEAD_DIM), lambda s, h, j=j: (0, j * n_heads + h)) for j in range(3)]
    tile_in = pl.BlockSpec((seq_len, HEAD_DIM), lambda s, h: (s, part * n_heads + h))
    table = pl.BlockSpec((seq_len, HEAD_DIM), lambda s, h: (0, 0))
    pairs = n_seq * n_heads * seq_len * seq_len
    head_buf = pltpu.VMEM((seq_len, HEAD_DIM), jnp.bfloat16)
    turned = pltpu.VMEM((HEAD_DIM, seq_len), jnp.float32)
    return pl.pallas_call(
        attn_kernel,
        grid=(n_seq, n_heads),
        in_specs=[*third, tile_in, table, table, *third_b],
        out_specs=[
            tile,
            pl.BlockSpec((seq_len, 3 * width), lambda s, h: (s, 0)),
            pl.BlockSpec((1, 8, 3 * width), lambda s, h: (s, 0, 0)),
        ],
        out_shape=[
            jax.ShapeDtypeStruct((tokens, width), jnp.bfloat16),
            jax.ShapeDtypeStruct((tokens, 3 * width), jnp.bfloat16),
            jax.ShapeDtypeStruct((n_seq, 8, 3 * width), jnp.float32),
        ],
        scratch_shapes=[head_buf, head_buf, head_buf, turned, turned],
        compiler_params=pltpu.CompilerParams(
            dimension_semantics=("arbitrary", "arbitrary"), vmem_limit_bytes=VMEM_MAX),
        cost_estimate=pl.CostEstimate(
            flops=6 * 2 * HEAD_DIM * pairs, bytes_accessed=22 * tokens * width, transcendentals=pairs),
        name="attn_fwd_bwd",
    )(lin, lin, lin, d_attn, cos_t, sin_t, bias, bias, bias)


def block_fwd_bwd(x_rows, hidden, inv_rms, grad_out, seq_len, gain_f, biases, w_groups, w_out, on_grad):
    f32 = jnp.float32
    tn = (((0,), (0,)), ((), ()))
    n_groups = len(w_groups)
    cos_t, sin_t = rope_tables(seq_len)
    x_full = x_rows.astype(f32)
    x_norm = x_full * inv_rms
    outs, d_lins, bias_grads, grad_ws = [], [], [], []
    hid = hidden
    d_attn = dot_nt(grad_out, w_out).astype(jnp.bfloat16)
    for g in range(n_groups):
        lin = dot_nn(hid, w_groups[g])
        o_g, d_lin, gb = attention(lin, d_attn, biases[g], cos_t, sin_t, g, n_groups)
        grad_w = lax.dot_general(hidden, d_lin, tn, preferred_element_type=f32)
        hid, grad_w = lax.optimization_barrier((hidden, grad_w))
        grad_ws.append(on_grad(grad_w))
        outs.append(o_g)
        d_lins.append(d_lin)
        bias_grads.append(jnp.sum(gb[:, 0], axis=0))
    attn_b = jnp.concatenate(outs, axis=1)
    grad_wo = on_grad(lax.dot_general(attn_b, grad_out, tn, preferred_element_type=f32))
    block_out = (x_full + dot_nn(attn_b, w_out)).astype(jnp.bfloat16)
    d_hidden = dot_nt(d_lins[0], w_groups[0])
    for g in range(1, n_groups):
        d_hidden = d_hidden + dot_nt(d_lins[g], w_groups[g])
    grad_gain = jnp.sum(d_hidden * x_norm, axis=0)
    d_norm = d_hidden * gain_f
    d_x = grad_out.astype(f32) + inv_rms * (d_norm - x_norm * jnp.mean(d_norm * x_norm, axis=-1, keepdims=True))
    return block_out, d_x, grad_ws, grad_wo, grad_gain, jnp.stack(bias_grads)


def barrier_all(me):
    barrier = pltpu.get_barrier_semaphore()
    for step in range(1, N_DEV):
        pl.semaphore_signal(barrier, inc=1, device_id=(jnp.bitwise_xor(me, step),), device_id_type=MESH)
    pl.semaphore_wait(barrier, N_DEV - 1)


LOOK_CHUNK = 64
LOOK_N = HOT // 2 // LOOK_CHUNK


def lookup_kernel(cold_ref, _, vec_ref, rows_ref, got_ref, vgot_ref,
                  recv_sem, link_sem, mate_sem, c_send, c_recv, v_send, v_recv, l_sem):
    me = lax.axis_index(AXIS)
    chip, core = me // 2, me % 2
    barrier_all(me)
    own = pltpu.make_async_copy(cold_ref.at[me], got_ref.at[me], l_sem.at[0])
    own_v = pltpu.make_async_copy(vec_ref, vgot_ref.at[me], l_sem.at[1])
    own.start()
    own_v.start()

    def cold_copy(step):
        peer = jnp.bitwise_xor(me, step)
        return pltpu.make_async_remote_copy(
            src_ref=cold_ref.at[peer], dst_ref=got_ref.at[me],
            send_sem=c_send.at[step - 1], recv_sem=c_recv.at[step - 1],
            device_id=(peer,), device_id_type=MESH)

    def vec_copy(step):
        peer = jnp.bitwise_xor(me, step)
        return pltpu.make_async_remote_copy(
            src_ref=vec_ref, dst_ref=vgot_ref.at[me], send_sem=v_send.at[step - 1], recv_sem=v_recv.at[step - 1],
            device_id=(peer,), device_id_type=MESH)

    def piece(part, k):
        return rows_ref.at[pl.ds(part * (HOT // 2) + k * LOOK_CHUNK, LOOK_CHUNK)]

    def link_copy(part, k, target):
        return pltpu.make_async_remote_copy(
            src_ref=piece(part, k), dst_ref=piece(part, k), send_sem=link_sem.at[part, k],
            recv_sem=recv_sem.at[part, k], device_id=(target,), device_id_type=MESH)

    def mate_copy(part, k):
        return pltpu.make_async_remote_copy(
            src_ref=piece(part, k), dst_ref=piece(part, k), send_sem=mate_sem.at[part, k],
            recv_sem=recv_sem.at[part, k], device_id=(jnp.bitwise_xor(me, 1),), device_id_type=MESH)

    place = [
        jnp.where(chip == 0, 0, jnp.where(chip == 1, 1, jnp.where(chip == 3, 2, 3))),
        jnp.where(chip == 0, 0, jnp.where(chip == 2, 1, jnp.where(chip == 3, 2, 3))),
    ]
    target = [
        2 * jnp.where(chip == 0, 1, jnp.where(chip == 1, 3, 2)),
        2 * jnp.where(chip == 0, 2, jnp.where(chip == 2, 3, 1)),
    ]

    def stage(step, carry):
        for part in range(2):
            k = step - place[part]
            live = (k >= 0) & (k < LOOK_N)

            @pl.when(live & (me != 0))
            def _():
                mate_copy(part, k).wait_recv()

            @pl.when(live & (core == 0) & (place[part] < 3))
            def _():
                link_copy(part, k, target[part]).start()

            @pl.when(live & (core == 0))
            def _():
                mate_copy(part, k).start()
        return carry

    def start_cold():
        for step in range(1, N_DEV):
            cold_copy(step).start()

    for step in range(1, N_DEV):
        vec_copy(step).start()
    pl.when(me != 0)(start_cold)
    lax.fori_loop(0, LOOK_N + 3, stage, 0)
    pl.when(me == 0)(start_cold)

    def drain(k, carry):
        for part in range(2):
            @pl.when((core == 0) & (place[part] < 3))
            def _():
                link_copy(part, k, target[part]).wait_send()

            @pl.when(core == 0)
            def _():
                mate_copy(part, k).wait_send()
        return carry

    lax.fori_loop(0, LOOK_N, drain, 0)
    for step in range(1, N_DEV):
        vec_copy(step).wait()
        cold_copy(step).wait()
    own.wait()
    own_v.wait()


def lookup_exchange(cold_send, hot_rows, vecs):
    any_spec = pl.BlockSpec(memory_space=pl.ANY)
    dma = pltpu.SemaphoreType.DMA
    return pl.pallas_call(
        lookup_kernel,
        out_shape=[
            jax.ShapeDtypeStruct(hot_rows.shape, hot_rows.dtype),
            jax.ShapeDtypeStruct(cold_send.shape, cold_send.dtype),
            jax.ShapeDtypeStruct((N_DEV,) + vecs.shape, vecs.dtype),
        ],
        in_specs=[any_spec] * 3,
        out_specs=[any_spec] * 3,
        scratch_shapes=[dma((2, LOOK_N))] * 3 + [dma((N_DEV - 1,))] * 4 + [dma((2,))],
        input_output_aliases={1: 0},
        compiler_params=pltpu.CompilerParams(collective_id=0, has_side_effects=True),
        name="lookup_exchange",
    )(cold_send, hot_rows, vecs)


def pick_kernel(idx_ref, hot_ref, cold_ref, gain_ref, x_ref, hid_ref, inv_ref, rows, picked, sem):
    step = pl.program_id(0)
    count, width = x_ref.shape
    base = step * count

    @pl.when(step == 0)
    def _():
        hot = pltpu.make_async_copy(hot_ref, rows.at[pl.ds(0, HOT)], sem.at[0])
        cold = pltpu.make_async_copy(cold_ref, rows.at[pl.ds(HOT, cold_ref.shape[0])], sem.at[1])
        hot.start()
        cold.start()
        hot.wait()
        cold.wait()

    def body(i8, carry):
        for j in range(8):
            i = i8 * 8 + j
            picked[i] = rows[idx_ref[base + i]]
        return carry

    lax.fori_loop(0, count // 8, body, 0)
    x = picked[...].reshape(count, width)
    x_ref[...] = x
    x_full = x.astype(jnp.float32)
    inv = lax.rsqrt(jnp.mean(x_full * x_full, axis=-1, keepdims=True) + NORM_EPS)
    inv_ref[...] = inv
    hid_ref[...] = (x_full * inv * gain_ref[...]).astype(jnp.bfloat16)


def pick_rows(idx, hot, cold, gain, block):
    count = idx.shape[0]
    tail = hot.shape[1:]
    width = tail[0] * tail[1]
    any_spec = pl.BlockSpec(memory_space=pl.ANY)
    wide = pl.BlockSpec((block, width), lambda i, s: (i, 0))
    act = jax.ShapeDtypeStruct((count, width), hot.dtype)
    return pl.pallas_call(
        pick_kernel,
        grid_spec=pltpu.PrefetchScalarGridSpec(
            num_scalar_prefetch=1,
            grid=(count // block,),
            in_specs=[any_spec, any_spec, pl.BlockSpec((1, width), lambda i, s: (0, 0))],
            out_specs=[wide, wide, pl.BlockSpec((block, 1), lambda i, s: (i, 0))],
            scratch_shapes=[
                pltpu.VMEM((hot.shape[0] + cold.shape[0],) + tail, hot.dtype),
                pltpu.VMEM((block,) + tail, hot.dtype),
                pltpu.SemaphoreType.DMA((2,)),
            ],
        ),
        out_shape=[act, act, jax.ShapeDtypeStruct((count, 1), jnp.float32)],
        compiler_params=pltpu.CompilerParams(dimension_semantics=("arbitrary",), vmem_limit_bytes=VMEM_MAX),
        name="pick_rows",
    )(idx, hot, cold, gain)


def take2d_kernel(idx_ref, idx2_ref, rows_ref, out_ref, out2_ref, buf):
    step = pl.program_id(0)

    def copy_rows(idx, dst, count):
        def body(i8, carry):
            for j in range(8):
                i = i8 * 8 + j
                dst[pl.ds(i, 1), :] = rows_ref[pl.ds(idx[step * count + i], 1), :]
            return carry

        lax.fori_loop(0, count // 8, body, 0)

    copy_rows(idx_ref, buf, buf.shape[0])
    out_ref[...] = buf[...].astype(out_ref.dtype)
    copy_rows(idx2_ref, out2_ref, out2_ref.shape[0])


def take2d(idx, idx2, rows, steps):
    count, count2 = idx.shape[0] // steps, idx2.shape[0] // steps
    width = rows.shape[1]
    return pl.pallas_call(
        take2d_kernel,
        grid_spec=pltpu.PrefetchScalarGridSpec(
            num_scalar_prefetch=2,
            grid=(steps,),
            in_specs=[pl.BlockSpec(rows.shape, lambda i, a, b: (0, 0), pipeline_mode=pl.Buffered(1))],
            out_specs=[
                pl.BlockSpec((count, width), lambda i, a, b: (i, 0)),
                pl.BlockSpec((count2, width), lambda i, a, b: (i, 0)),
            ],
            scratch_shapes=[pltpu.VMEM((count, width), jnp.float32)],
        ),
        out_shape=[
            jax.ShapeDtypeStruct((count * steps, width), jnp.bfloat16),
            jax.ShapeDtypeStruct((count2 * steps, width), jnp.float32),
        ],
        compiler_params=pltpu.CompilerParams(dimension_semantics=("arbitrary",), vmem_limit_bytes=VMEM_MAX),
        name="take_rows",
    )(idx, idx2, rows)


def seg_sum_kernel(key_ref, off_ref, mine_ref, mate_ref, out_ref, src, sem):
    blk = pl.program_id(0)
    count = mine_ref.shape[0]

    @pl.when(blk == 0)
    def _():
        first = pltpu.make_async_copy(mine_ref, src.at[pl.ds(0, count)], sem.at[0])
        second = pltpu.make_async_copy(mate_ref, src.at[pl.ds(count, count)], sem.at[1])
        first.start()
        second.start()
        first.wait()
        second.wait()

    out_ref[...] = jnp.zeros_like(out_ref)

    def body(e, carry):
        key = key_ref[e]
        row = lax.shift_right_logical(key, 12) - blk * ROW_BLOCK
        tok = jnp.bitwise_and(key, 4095)
        out_ref[pl.ds(row, 1), :] += src[pl.ds(tok, 1), :]
        return carry

    lax.fori_loop(off_ref[blk], off_ref[blk + 1], body, 0)


def seg_sum(keys, offs, dx_mine, dx_mate, n_rows):
    tokens, width = dx_mine.shape
    any_spec = pl.BlockSpec(memory_space=pl.ANY)
    return pl.pallas_call(
        seg_sum_kernel,
        grid_spec=pltpu.PrefetchScalarGridSpec(
            num_scalar_prefetch=2,
            grid=(n_rows // ROW_BLOCK,),
            in_specs=[any_spec, any_spec],
            out_specs=pl.BlockSpec((ROW_BLOCK, width), lambda i, a, b: (i, 0)),
            scratch_shapes=[pltpu.VMEM((2 * tokens, width), jnp.float32), pltpu.SemaphoreType.DMA((2,))],
        ),
        out_shape=jax.ShapeDtypeStruct((n_rows, width), jnp.float32),
        compiler_params=pltpu.CompilerParams(dimension_semantics=("arbitrary",), vmem_limit_bytes=VMEM_MAX),
        name="hot_seg_sum",
    )(keys, offs, dx_mine, dx_mate)


RED_CHUNK = 32
RED_N = HOT // 2 // RED_CHUNK


def reduce_kernel(part_ref, cold_ref, more_ref, vec_ref, hot_ref, crecv_ref, mrecv_ref, vrecv_ref,
                  local, incoming, load_sem, send_sem, recv_sem, out_sem,
                  c_send, c_recv, m_send, m_recv, v_send, v_recv, l_sem):
    me = lax.axis_index(AXIS)
    chip, core = me // 2, me % 2
    mid = jnp.where(core == 0, 1, 2)
    first = 3 - mid
    place = jnp.where(chip == first, 0, jnp.where(chip == 3, 1, jnp.where(chip == mid, 2, 3)))
    nxt = jnp.where(chip == first, 3, jnp.where(chip == 3, mid, 0))
    target = nxt * 2 + core

    def rows(k):
        return pl.ds(k * RED_CHUNK, RED_CHUNK)

    def load(k):
        return pltpu.make_async_copy(part_ref.at[rows(k)], local.at[rows(k)], load_sem.at[k])

    def send(k):
        return pltpu.make_async_remote_copy(
            src_ref=local.at[rows(k)], dst_ref=incoming.at[rows(k)], send_sem=send_sem.at[k],
            recv_sem=recv_sem.at[k], device_id=(target,), device_id_type=MESH)

    def put_own(k):
        return pltpu.make_async_copy(local.at[rows(k)], hot_ref.at[rows(k)], send_sem.at[k])

    def put_far(k):
        return pltpu.make_async_remote_copy(
            src_ref=local.at[rows(k)], dst_ref=hot_ref.at[pl.ds(HOT // 2 + k * RED_CHUNK, RED_CHUNK)],
            send_sem=send_sem.at[k], recv_sem=out_sem.at[k], device_id=(jnp.bitwise_xor(me, 1),), device_id_type=MESH)

    swaps = (
        (vec_ref, vrecv_ref, v_send, v_recv),
        (more_ref, mrecv_ref, m_send, m_recv),
        (cold_ref, crecv_ref, c_send, c_recv),
    )

    def swap(which, step):
        src, dst, s_sem, r_sem = swaps[which]
        peer = jnp.bitwise_xor(me, step)
        return pltpu.make_async_remote_copy(
            src_ref=src.at[peer], dst_ref=dst.at[me], send_sem=s_sem.at[step - 1], recv_sem=r_sem.at[step - 1],
            device_id=(peer,), device_id_type=MESH)

    def keep(which):
        src, dst, _, _ = swaps[which]
        return pltpu.make_async_copy(src.at[me], dst.at[me], l_sem.at[which])

    def start_load(k, carry):
        load(k).start()
        return carry

    lax.fori_loop(0, RED_N, start_load, 0)
    barrier_all(me)
    for which in range(3):
        keep(which).start()
    for which in range(2):
        for step in range(1, N_DEV):
            swap(which, step).start()

    def cold_at(k, step):
        return jnp.where(place >= 2, k == 0, k == 4 * step)

    def stage(k, carry):
        @pl.when(k < RED_N)
        def _():
            load(k).wait()

        @pl.when((k < RED_N) & (place > 0))
        def _():
            send(k).wait_recv()
            local[rows(k), :] += incoming[rows(k), :]

        @pl.when((k >= 1) & (place < 3))
        def _():
            send(k - 1).start()

        for step in range(1, N_DEV):
            @pl.when(cold_at(k, step))
            def _():
                swap(2, step).start()

        @pl.when((k >= 1) & (me == 0))
        def _():
            put_own(k - 1).start()

        @pl.when((k >= 1) & (me == 1))
        def _():
            put_far(k - 1).start()
        return carry

    lax.fori_loop(0, RED_N + 1, stage, 0)

    def drain(k, carry):
        @pl.when(place < 3)
        def _():
            send(k).wait_send()

        @pl.when(me == 0)
        def _():
            put_own(k).wait()
            put_far(k).wait_recv()

        @pl.when(me == 1)
        def _():
            put_far(k).wait_send()
        return carry

    lax.fori_loop(0, RED_N, drain, 0)
    for which in range(3):
        for step in range(1, N_DEV):
            swap(which, step).wait()
        keep(which).wait()


def grad_exchange(part, cold_send, more_send, vecs):
    any_spec = pl.BlockSpec(memory_space=pl.ANY)
    dma = pltpu.SemaphoreType.DMA
    width = part.shape[1]
    return pl.pallas_call(
        reduce_kernel,
        out_shape=[jax.ShapeDtypeStruct((HOT, width), jnp.float32)]
        + [jax.ShapeDtypeStruct(a.shape, a.dtype) for a in (cold_send, more_send, vecs)],
        in_specs=[any_spec] * 4,
        out_specs=[any_spec] * 4,
        scratch_shapes=[pltpu.VMEM(part.shape, jnp.float32)] * 2
        + [dma((RED_N,))] * 4 + [dma((N_DEV - 1,))] * 6 + [dma((3,))],
        compiler_params=pltpu.CompilerParams(
            collective_id=1, has_side_effects=True, vmem_limit_bytes=VMEM_MAX),
        name="grad_exchange",
    )(part, cold_send, more_send, vecs)


def table_kernel(key_ref, off_ref, n_hot_ref, src_ref, more_ref, hot_ref, out_ref, acc, rows, half_rows, sem):
    blk = pl.program_id(0)
    n_src = src_ref.shape[0]

    @pl.when(blk == 0)
    def _():
        low = pltpu.make_async_copy(src_ref, half_rows, sem.at[0])
        high = pltpu.make_async_copy(more_ref, rows.at[pl.ds(n_src, more_ref.shape[0])], sem.at[1])
        low.start()
        high.start()
        low.wait()
        for c in range(N_DEV):
            part = pl.ds(c * (n_src // N_DEV), n_src // N_DEV)
            rows[part, :] = half_rows[part, :].astype(jnp.float32)
        high.wait()

    is_hot = blk < n_hot_ref[0]

    @pl.when(is_hot)
    def _():
        acc[...] = hot_ref[...]

    @pl.when(jnp.logical_not(is_hot))
    def _():
        acc[...] = jnp.zeros_like(acc)

    def body(e, carry):
        key = key_ref[e]
        row = lax.shift_right_logical(key, 11) - blk * TABLE_BLOCK
        idx = jnp.bitwise_and(key, 2047)
        acc[pl.ds(row, 1), :] += rows[pl.ds(idx, 1), :]
        return carry

    lax.fori_loop(off_ref[blk], off_ref[blk + 1], body, 0)
    out_ref[...] = acc[...].astype(out_ref.dtype)


def build_table(keys, offs, n_hot, src, more, hot, n_rows):
    width = src.shape[1]

    def hot_index(i, k, o, n):
        return (jnp.minimum(i, jnp.maximum(n[0] - 1, 0)), 0)

    return pl.pallas_call(
        table_kernel,
        grid_spec=pltpu.PrefetchScalarGridSpec(
            num_scalar_prefetch=3,
            grid=(pl.cdiv(n_rows, TABLE_BLOCK),),
            in_specs=[
                pl.BlockSpec(memory_space=pl.ANY),
                pl.BlockSpec(memory_space=pl.ANY),
                pl.BlockSpec((TABLE_BLOCK, width), hot_index),
            ],
            out_specs=pl.BlockSpec((TABLE_BLOCK, width), lambda i, k, o, n: (i, 0)),
            scratch_shapes=[
                pltpu.VMEM((TABLE_BLOCK, width), jnp.float32),
                pltpu.VMEM((src.shape[0] + more.shape[0], width), jnp.float32),
                pltpu.VMEM(src.shape, src.dtype),
                pltpu.SemaphoreType.DMA((2,)),
            ],
        ),
        out_shape=jax.ShapeDtypeStruct((n_rows, width), jnp.bfloat16),
        compiler_params=pltpu.CompilerParams(dimension_semantics=("arbitrary",), vmem_limit_bytes=VMEM_MAX),
        name="build_table",
    )(keys, offs, n_hot, src, more, hot)


def lookup_plan(all_ids, own_ids, me, rows_dev):
    tokens = own_ids.shape[0]
    t_idx = jnp.arange(tokens, dtype=jnp.int32)
    devices = jnp.arange(N_DEV, dtype=jnp.int32)
    first_row = me * rows_dev
    mine = (all_ids >= HOT) & (all_ids >= first_row) & (all_ids < first_row + rows_dev)
    key = first_of(mine, t_idx[None, :] * 32768 + (all_ids - first_row), CAP)
    ask_row = jnp.where(key != BIG, jnp.bitwise_and(key, 32767), 0).reshape(-1)
    hit = (own_ids // rows_dev == devices[:, None]) & (own_ids >= HOT)[None, :]
    place = jnp.cumsum(hit.astype(jnp.int32), axis=1) - 1 + devices[:, None] * CAP
    idx = jnp.where(own_ids >= HOT, HOT + jnp.sum(jnp.where(hit, place, 0), axis=0), own_ids)
    return ask_row, idx


def fast_lookup(ask_row, idx, table_part, gain_vecs):
    width = table_part.shape[1]
    send = jnp.take(table_part, ask_row, axis=0, mode="clip")
    tiles = (width // LANES, LANES)
    send = send.reshape((N_DEV, CAP) + tiles)
    hot, cold, vecs = lookup_exchange(send, table_part[:HOT].reshape((HOT,) + tiles), gain_vecs)
    vecs = vecs.transpose(1, 0, 2).reshape(gain_vecs.shape[0], -1).astype(jnp.float32)
    normed = pick_rows(idx, hot, cold.reshape((N_DEV * CAP,) + tiles), vecs[:1], 256)
    return normed, cold, vecs


def first_of(mask, values, count):
    return lax.sort(jnp.where(mask, values, BIG), dimension=1)[:, :count]


def repeats(all_ids):
    flat = all_ids.reshape(-1).astype(jnp.uint32)
    pos = jnp.arange(flat.shape[0], dtype=jnp.uint32)
    ordered = lax.sort(flat * jnp.uint32(16384) + pos)
    ident = ordered // jnp.uint32(16384)
    same = ident[1:] == ident[:-1]
    no = jnp.zeros((1,), jnp.bool_)
    again = jnp.concatenate([no, same]) | jnp.concatenate([same, no])
    again = lax.sort((ordered % jnp.uint32(16384)) * jnp.uint32(2) + again.astype(jnp.uint32)) % jnp.uint32(2)
    return (again == 1).reshape(all_ids.shape)


def grad_plan(all_ids, own_ids, again, me, rows_dev):
    tokens = own_ids.shape[0]
    t_idx = jnp.arange(tokens, dtype=jnp.int32)[None, :]
    devices = jnp.arange(N_DEV, dtype=jnp.int32)
    owners = jnp.where(all_ids >= HOT, all_ids // rows_dev, -1)
    hit = lax.dynamic_index_in_dim(owners, me, 0, keepdims=False)[None, :] == devices[:, None]
    own_again = lax.dynamic_index_in_dim(again, me, 0, keepdims=True)
    slot_tok = first_of(hit, t_idx, CAP)
    more_tok = first_of(hit & own_again, t_idx, MORE)
    mine = owners == me
    local = all_ids - me * rows_dev
    row = first_of(mine, t_idx * 65536 + local * 2 + again, CAP)
    more_row = first_of(mine & again, t_idx * 65536 + local * 2 + again, MORE)
    slots = jnp.arange(N_DEV * CAP, dtype=jnp.int32).reshape(N_DEV, CAP)
    more_slots = N_DEV * CAP + jnp.arange(N_DEV * MORE, dtype=jnp.int32).reshape(N_DEV, MORE)

    def owner_key(packed, slot, wanted):
        where = jnp.bitwise_and(lax.shift_right_logical(packed, 1), 32767)
        return jnp.where((packed != BIG) & (jnp.bitwise_and(packed, 1) == wanted), where * 2048 + slot, BIG).reshape(-1)

    owner_keys = lax.sort(jnp.concatenate([owner_key(row, slots, 0), owner_key(more_row, more_slots, 1)]))

    def clean(tok):
        return jnp.where(tok == BIG, 0, tok).reshape(-1)

    return clean(slot_tok), clean(more_tok), owner_keys


def block_offsets(keys, n_blocks, block, shift):
    edges = jnp.arange(n_blocks + 1, dtype=jnp.int32) * (block << shift)
    return jnp.sum(keys[None, :] < edges[:, None], axis=1).astype(jnp.int32)


def fast_table_grad(rows_dev, all_ids, own_ids, d_x, vecs, slot_tok, more_tok, owner_keys):
    tokens, width = d_x.shape
    me = lax.axis_index(AXIS)
    mate_of = [(i, i ^ 1) for i in range(N_DEV)]
    dx_mate = lax.ppermute(d_x, AXIS, mate_of)
    mate_ids = lax.dynamic_index_in_dim(all_ids, jnp.bitwise_xor(me, 1), 0, keepdims=False)
    pair_ids = jnp.concatenate([own_ids, mate_ids])
    base = (me % 2) * (HOT // 2)
    inside = (pair_ids >= base) & (pair_ids < base + HOT // 2)
    keys = jnp.where(inside, (pair_ids - base) * 4096 + jnp.arange(2 * tokens, dtype=jnp.int32), BIG)
    keys = lax.sort(keys)
    part = seg_sum(keys, block_offsets(keys, HOT // 2 // ROW_BLOCK, ROW_BLOCK, 12), d_x, dx_mate, HOT // 2)
    cold, more = take2d(slot_tok, more_tok, d_x, N_DEV)
    cold = cold.reshape(N_DEV, CAP, width)
    more = more.reshape(N_DEV, MORE, width)
    hot, recv, more_recv, vec_recv = grad_exchange(part, cold, more, vecs)
    n_hot = jnp.where(me == 0, HOT // TABLE_BLOCK, 0).astype(jnp.int32)[None]
    offs = block_offsets(owner_keys, pl.cdiv(rows_dev, TABLE_BLOCK), TABLE_BLOCK, 11)
    recv = recv.reshape(N_DEV * CAP, width)
    more_recv = more_recv.reshape(N_DEV * MORE, width)
    grad_part = build_table(owner_keys, offs, n_hot, recv, more_recv, hot, rows_dev)
    return grad_part, jnp.sum(vec_recv, axis=0)


def slow_lookup(all_ids, table_part, me):
    rows_dev = table_part.shape[0]
    local_idx = all_ids - me * rows_dev
    is_owned = (local_idx >= 0) & (local_idx < rows_dev)
    looked = jnp.take(table_part, jnp.where(is_owned, local_idx, 0), axis=0)
    looked = jnp.where(is_owned[..., None], looked, jnp.zeros((), jnp.bfloat16))
    return lax.psum_scatter(looked, AXIS, scatter_dimension=0)


def slow_table_grad(rows_dev, all_ids, d_x, vecs):
    me = lax.axis_index(AXIS)
    local_idx = all_ids - me * rows_dev
    is_owned = (local_idx >= 0) & (local_idx < rows_dev)
    all_dx = lax.all_gather(d_x, AXIS)
    seg_idx = jnp.where(is_owned, local_idx, rows_dev)
    grad_part = jax.ops.segment_sum(all_dx.reshape(-1, d_x.shape[-1]), seg_idx.reshape(-1), num_segments=rows_dev)
    return grad_part.astype(jnp.bfloat16), lax.psum_scatter(vecs, AXIS, scatter_dimension=0)


def solution(mesh):
    row_spec = P(AXIS, None)
    vec_spec = P(AXIS)
    act_spec = P(AXIS, None, None)
    weight_specs = (vec_spec, row_spec, vec_spec, row_spec, vec_spec, row_spec, vec_spec, row_spec)
    in_specs = (row_spec, act_spec, row_spec) + weight_specs
    out_specs = (act_spec, row_spec) + weight_specs

    def run(fast, tok_ids, all_ids, again, ask_row, idx, grad_out, table_part, gain_part, wq_part, bq_part, wk_part, bk_part, wv_part, bv_part, wo_part):
        me = lax.axis_index(AXIS)
        rows_dev, width = table_part.shape
        n_seq, seq_len = tok_ids.shape
        own_ids = tok_ids.reshape(-1)

        def whole(part):
            return lax.all_gather(part, AXIS, axis=0, tiled=True)

        def scatter(grad):
            return lax.psum_scatter(grad, AXIS, scatter_dimension=0, tiled=True)

        part_w = gain_part.shape[0]
        group = wq_part.shape[1] // GROUPS
        cols = [slice(g * group, (g + 1) * group) for g in range(GROUPS)]
        vec_parts = jnp.pad(jnp.stack([gain_part, bq_part, bk_part, bv_part]), ((0, 12), (0, 0)))
        w_parts = [jnp.concatenate([wq_part[:, c], wk_part[:, c], wv_part[:, c]], axis=1) for c in cols]
        if fast:
            (x_rows, hidden, inv_rms), marker, vec_full = fast_lookup(ask_row, idx, table_part, vec_parts)
            late = lax.optimization_barrier((marker, all_ids, own_ids, again, wo_part, *w_parts[1:]))
            plan_ids, wo_part, w_parts = late[1:4], late[4], [w_parts[0], *late[5:]]
        else:
            x_rows = slow_lookup(all_ids, table_part, me)
            vec_full = lax.all_gather(vec_parts, AXIS, axis=1, tiled=True).astype(jnp.float32)
            x_full = x_rows.astype(jnp.float32)
            inv_rms = lax.rsqrt(jnp.mean(x_full * x_full, axis=-1, keepdims=True) + NORM_EPS)
            hidden = (x_full * inv_rms * vec_full[0]).astype(jnp.bfloat16)
        biases = [jnp.concatenate([vec_full[1, c], vec_full[2, c], vec_full[3, c]])[None] for c in cols]
        wo_full = whole(wo_part)
        w_groups = [whole(part) for part in w_parts]
        grad_flat = grad_out.reshape(-1, width)
        block_out, d_x, grad_ws, grad_wo, grad_gain, grad_bias = block_fwd_bwd(
            x_rows, hidden, inv_rms, grad_flat, seq_len, vec_full[0], biases, w_groups, wo_full, scatter)
        gq, gk, gv = (
            jnp.concatenate([grad_w[:, j * group:(j + 1) * group] for grad_w in grad_ws], axis=1) for j in range(3))
        grad_bias = grad_bias.reshape(GROUPS, 3, group)
        vecs = jnp.stack([grad_gain] + [grad_bias[:, j].reshape(-1) for j in range(3)])
        vecs = jnp.pad(vecs.reshape(4, N_DEV, part_w).transpose(1, 0, 2), ((0, 0), (0, 4), (0, 0)))
        rest = (all_ids, own_ids, d_x, vecs)
        if fast:
            grad_part, vec_sum = fast_table_grad(rows_dev, *rest, *grad_plan(*plan_ids, me, rows_dev))
        else:
            grad_part, vec_sum = slow_table_grad(rows_dev, all_ids, d_x, vecs)
        return (block_out.reshape(grad_out.shape), grad_part, vec_sum[0], gq, vec_sum[1], gk, vec_sum[2], gv, vec_sum[3], grad_wo)

    def device_step(tok_ids, grad_out, table_part, *weights):
        rows_dev = table_part.shape[0]
        all_ids = lax.all_gather(tok_ids.reshape(-1), AXIS)
        me = lax.axis_index(AXIS)
        again = repeats(all_ids)
        owners = jnp.where(all_ids >= HOT, all_ids // rows_dev, -1)
        asked = owners[None] == jnp.arange(N_DEV, dtype=jnp.int32)[:, None, None]
        counts = jnp.sum(asked.astype(jnp.int32), axis=-1)
        more = jnp.sum((asked & again[None]).astype(jnp.int32), axis=-1)
        fits = (jnp.max(counts) <= CAP) & (jnp.max(more) <= MORE)
        ask_row, idx = lookup_plan(all_ids, tok_ids.reshape(-1), me, rows_dev)
        args = (tok_ids, all_ids, again, ask_row, idx, grad_out, table_part) + weights
        return lax.cond(fits, functools.partial(run, True), functools.partial(run, False), *args)

    return jax.shard_map(device_step, mesh=mesh, in_specs=in_specs, out_specs=out_specs, check_vma=False)
```

```python
import functools

import jax
import jax.numpy as jnp
from jax import lax
from jax.experimental import pallas as pl
from jax.experimental.pallas import tpu as pltpu
from jax.sharding import PartitionSpec as P

HEAD_DIM = 128
ROPE_THETA = 1.0e6
NORM_EPS = 1e-6
MASK_VALUE = -1e30
AXIS = "fsdp"
N_DEV = 8
HOT = 4096
CAP = 176
MORE = 24
LANES = 128
BIG = 2**31 - 1
MESH = pl.DeviceIdType.MESH
BLOCK_Q = 512
GROUPS = 4
ROW_BLOCK = 128
TABLE_BLOCK = 512
VMEM_MAX = 60 * 1024 * 1024


def dot_nn(a, b):
    return lax.dot_general(a, b, (((1,), (0,)), ((), ())), preferred_element_type=jnp.float32)


def dot_nt(a, b):
    return lax.dot_general(a, b, (((1,), (1,)), ((), ())), preferred_element_type=jnp.float32)


def attn_kernel(q_ref, k_ref, v_ref, do_ref, cos_ref, sin_ref, bq_ref, bk_ref, bv_ref,
                o_ref, dlin_ref, gb_ref, qs, ks, vs, dkt, dvt):
    seq_len = q_ref.shape[0]
    start = pl.program_id(1) * HEAD_DIM
    third = dlin_ref.shape[1] // 3
    q_cols, k_cols, v_cols = (pl.ds(pl.multiple_of(start + j * third, HEAD_DIM), HEAD_DIM) for j in range(3))
    score_scale = HEAD_DIM ** -0.5
    cos_t = cos_ref[...]
    sin_t = sin_ref[...]
    half = HEAD_DIM // 2
    q_lin = q_ref[...] + bq_ref[...]
    qs[...] = (q_lin * cos_t + pltpu.roll(q_lin, half, 1) * sin_t).astype(jnp.bfloat16)
    k_lin = k_ref[...] + bk_ref[...]
    ks[...] = (k_lin * cos_t + pltpu.roll(k_lin, half, 1) * sin_t).astype(jnp.bfloat16)
    vs[...] = (v_ref[...] + bv_ref[...]).astype(jnp.bfloat16)
    row_i = lax.broadcasted_iota(jnp.int32, (BLOCK_Q, BLOCK_Q), 0)
    col_i = lax.broadcasted_iota(jnp.int32, (BLOCK_Q, BLOCK_Q), 1)
    causal = row_i >= col_i
    n_blocks = seq_len // BLOCK_Q
    gbq = jnp.zeros((1, HEAD_DIM), jnp.float32)
    for blk in reversed(range(n_blocks)):
        lo = blk * BLOCK_Q
        width = lo + BLOCK_Q
        q_b = qs[pl.ds(lo, BLOCK_Q), :]
        do_b = do_ref[pl.ds(lo, BLOCK_Q), :]
        k_all = ks[pl.ds(0, width), :]
        v_all = vs[pl.ds(0, width), :]
        scores = dot_nt(q_b, k_all) * score_scale
        tail = jnp.where(causal, scores[:, lo:], MASK_VALUE)
        scores = jnp.concatenate([scores[:, :lo], tail], axis=1) if lo else tail
        top = jnp.max(scores, axis=1, keepdims=True)
        prob = jnp.exp(scores - top)
        prob = prob * (1.0 / jnp.sum(prob, axis=1, keepdims=True))
        prob_b = prob.astype(jnp.bfloat16)
        o_ref[pl.ds(lo, BLOCK_Q), :] = dot_nn(prob_b, v_all).astype(jnp.bfloat16)
        d_prob = dot_nt(do_b, v_all)
        inner = jnp.sum(d_prob * prob, axis=1, keepdims=True)
        d_score = ((prob * (d_prob - inner)) * score_scale).astype(jnp.bfloat16)
        d_q = dot_nn(d_score, k_all)
        scaled = d_q * sin_ref[pl.ds(lo, BLOCK_Q), :]
        d_q = d_q * cos_ref[pl.ds(lo, BLOCK_Q), :] + pltpu.roll(scaled, half, 1)
        gbq = gbq + jnp.sum(d_q, axis=0, keepdims=True)
        dlin_ref[pl.ds(lo, BLOCK_Q), q_cols] = d_q.astype(jnp.bfloat16)
        dv_part = dot_nn(do_b.T, prob_b)
        dk_part = dot_nn(q_b.T, d_score)
        if blk == n_blocks - 1:
            dvt[...] = dv_part
            dkt[...] = dk_part
        else:
            dvt[:, pl.ds(0, width)] += dv_part
            dkt[:, pl.ds(0, width)] += dk_part
    d_v = dvt[...].T
    d_k = dkt[...].T
    d_k = d_k * cos_t + pltpu.roll(d_k * sin_t, half, 1)
    dlin_ref[:, v_cols] = d_v.astype(jnp.bfloat16)
    dlin_ref[:, k_cols] = d_k.astype(jnp.bfloat16)
    gb_ref[0, 0:1, q_cols] = gbq
    gb_ref[0, 0:1, k_cols] = jnp.sum(d_k, axis=0, keepdims=True)
    gb_ref[0, 0:1, v_cols] = jnp.sum(d_v, axis=0, keepdims=True)


def rope_tables(seq_len):
    half = HEAD_DIM // 2
    inv_freq = jnp.power(ROPE_THETA, -(jnp.arange(half, dtype=jnp.float32) * 2.0 / HEAD_DIM))
    angles = jnp.arange(seq_len, dtype=jnp.float32)[:, None] * inv_freq[None, :]
    cos_t = jnp.concatenate([jnp.cos(angles)] * 2, axis=-1)
    sin_t = jnp.concatenate([-jnp.sin(angles), jnp.sin(angles)], axis=-1)
    return cos_t, sin_t


def attention(lin, d_attn, bias, cos_t, sin_t, part, parts):
    tokens = lin.shape[0]
    width = d_attn.shape[1] // parts
    seq_len = cos_t.shape[0]
    n_seq, n_heads = tokens // seq_len, width // HEAD_DIM
    tile = pl.BlockSpec((seq_len, HEAD_DIM), lambda s, h: (s, h))
    third = [pl.BlockSpec((seq_len, HEAD_DIM), lambda s, h, j=j: (s, j * n_heads + h)) for j in range(3)]
    third_b = [pl.BlockSpec((1, HEAD_DIM), lambda s, h, j=j: (0, j * n_heads + h)) for j in range(3)]
    tile_in = pl.BlockSpec((seq_len, HEAD_DIM), lambda s, h: (s, part * n_heads + h))
    table = pl.BlockSpec((seq_len, HEAD_DIM), lambda s, h: (0, 0))
    pairs = n_seq * n_heads * seq_len * seq_len
    head_buf = pltpu.VMEM((seq_len, HEAD_DIM), jnp.bfloat16)
    turned = pltpu.VMEM((HEAD_DIM, seq_len), jnp.float32)
    return pl.pallas_call(
        attn_kernel,
        grid=(n_seq, n_heads),
        in_specs=[*third, tile_in, table, table, *third_b],
        out_specs=[
            tile,
            pl.BlockSpec((seq_len, 3 * width), lambda s, h: (s, 0)),
            pl.BlockSpec((1, 8, 3 * width), lambda s, h: (s, 0, 0)),
        ],
        out_shape=[
            jax.ShapeDtypeStruct((tokens, width), jnp.bfloat16),
            jax.ShapeDtypeStruct((tokens, 3 * width), jnp.bfloat16),
            jax.ShapeDtypeStruct((n_seq, 8, 3 * width), jnp.float32),
        ],
        scratch_shapes=[head_buf, head_buf, head_buf, turned, turned],
        compiler_params=pltpu.CompilerParams(
            dimension_semantics=("arbitrary", "arbitrary"), vmem_limit_bytes=VMEM_MAX),
        cost_estimate=pl.CostEstimate(
            flops=6 * 2 * HEAD_DIM * pairs, bytes_accessed=22 * tokens * width, transcendentals=pairs),
        name="attn_fwd_bwd",
    )(lin, lin, lin, d_attn, cos_t, sin_t, bias, bias, bias)


def block_fwd_bwd(x_rows, hidden, inv_rms, grad_out, seq_len, gain_f, biases, w_groups, w_out, on_grad):
    f32 = jnp.float32
    tn = (((0,), (0,)), ((), ()))
    n_groups = len(w_groups)
    cos_t, sin_t = rope_tables(seq_len)
    x_full = x_rows.astype(f32)
    x_norm = x_full * inv_rms
    outs, d_lins, bias_grads, grad_ws = [], [], [], []
    hid = hidden
    d_attn = dot_nt(grad_out, w_out).astype(jnp.bfloat16)
    for g in range(n_groups):
        lin = dot_nn(hid, w_groups[g])
        o_g, d_lin, gb = attention(lin, d_attn, biases[g], cos_t, sin_t, g, n_groups)
        grad_w = lax.dot_general(hidden, d_lin, tn, preferred_element_type=f32)
        hid, grad_w = lax.optimization_barrier((hidden, grad_w))
        grad_ws.append(on_grad(grad_w))
        outs.append(o_g)
        d_lins.append(d_lin)
        bias_grads.append(jnp.sum(gb[:, 0], axis=0))
    attn_b = jnp.concatenate(outs, axis=1)
    grad_wo = on_grad(lax.dot_general(attn_b, grad_out, tn, preferred_element_type=f32))
    block_out = (x_full + dot_nn(attn_b, w_out)).astype(jnp.bfloat16)
    d_hidden = dot_nt(d_lins[0], w_groups[0])
    for g in range(1, n_groups):
        d_hidden = d_hidden + dot_nt(d_lins[g], w_groups[g])
    grad_gain = jnp.sum(d_hidden * x_norm, axis=0)
    d_norm = d_hidden * gain_f
    d_x = grad_out.astype(f32) + inv_rms * (d_norm - x_norm * jnp.mean(d_norm * x_norm, axis=-1, keepdims=True))
    return block_out, d_x, grad_ws, grad_wo, grad_gain, jnp.stack(bias_grads)


def barrier_all(me):
    barrier = pltpu.get_barrier_semaphore()
    for step in range(1, N_DEV):
        pl.semaphore_signal(barrier, inc=1, device_id=(jnp.bitwise_xor(me, step),), device_id_type=MESH)
    pl.semaphore_wait(barrier, N_DEV - 1)


LOOK_CHUNK = 64
LOOK_LAG = 4
LOOK_N = HOT // 2 // LOOK_CHUNK


def lookup_kernel(cold_ref, _, vec_ref, rows_ref, got_ref, vgot_ref,
                  recv_sem, link_sem, mate_sem, c_send, c_recv, v_send, v_recv, l_sem):
    me = lax.axis_index(AXIS)
    chip, core = me // 2, me % 2
    barrier_all(me)
    own = pltpu.make_async_copy(cold_ref.at[me], got_ref.at[me], l_sem.at[0])
    own_v = pltpu.make_async_copy(vec_ref, vgot_ref.at[me], l_sem.at[1])
    own.start()
    own_v.start()

    def cold_copy(step):
        peer = jnp.bitwise_xor(me, step)
        return pltpu.make_async_remote_copy(
            src_ref=cold_ref.at[peer], dst_ref=got_ref.at[me],
            send_sem=c_send.at[step - 1], recv_sem=c_recv.at[step - 1],
            device_id=(peer,), device_id_type=MESH)

    def vec_copy(step):
        peer = jnp.bitwise_xor(me, step)
        return pltpu.make_async_remote_copy(
            src_ref=vec_ref, dst_ref=vgot_ref.at[me], send_sem=v_send.at[step - 1], recv_sem=v_recv.at[step - 1],
            device_id=(peer,), device_id_type=MESH)

    def piece(part, k):
        return rows_ref.at[pl.ds(part * (HOT // 2) + k * LOOK_CHUNK, LOOK_CHUNK)]

    def link_copy(part, k, target):
        return pltpu.make_async_remote_copy(
            src_ref=piece(part, k), dst_ref=piece(part, k), send_sem=link_sem.at[part, k],
            recv_sem=recv_sem.at[part, k], device_id=(target,), device_id_type=MESH)

    def mate_copy(part, k):
        return pltpu.make_async_remote_copy(
            src_ref=piece(part, k), dst_ref=piece(part, k), send_sem=mate_sem.at[part, k],
            recv_sem=recv_sem.at[part, k], device_id=(jnp.bitwise_xor(me, 1),), device_id_type=MESH)

    place = [
        jnp.where(chip == 0, 0, jnp.where(chip == 1, 1, jnp.where(chip == 3, 2, 3))),
        jnp.where(chip == 0, 0, jnp.where(chip == 2, 1, jnp.where(chip == 3, 2, 3))),
    ]
    target = [
        2 * jnp.where(chip == 0, 1, jnp.where(chip == 1, 3, 2)),
        2 * jnp.where(chip == 0, 2, jnp.where(chip == 2, 3, 1)),
    ]

    def stage(step, carry):
        for part in range(2):
            k = step - LOOK_LAG * place[part]
            live = (k >= 0) & (k < LOOK_N)

            @pl.when(live & (me != 0))
            def _():
                mate_copy(part, k).wait_recv()

            @pl.when(live & (core == 0) & (place[part] < 3))
            def _():
                link_copy(part, k, target[part]).start()

            @pl.when(live & (core == 0))
            def _():
                mate_copy(part, k).start()
        return carry

    def start_cold():
        for step in range(1, N_DEV):
            cold_copy(step).start()

    for step in range(1, N_DEV):
        vec_copy(step).start()
    pl.when(me != 0)(start_cold)
    lax.fori_loop(0, LOOK_N + 3 * LOOK_LAG, stage, 0)
    pl.when(me == 0)(start_cold)

    def drain(k, carry):
        for part in range(2):
            @pl.when((core == 0) & (place[part] < 3))
            def _():
                link_copy(part, k, target[part]).wait_send()

            @pl.when(core == 0)
            def _():
                mate_copy(part, k).wait_send()
        return carry

    lax.fori_loop(0, LOOK_N, drain, 0)
    for step in range(1, N_DEV):
        vec_copy(step).wait()
        cold_copy(step).wait()
    own.wait()
    own_v.wait()


def lookup_exchange(cold_send, hot_rows, vecs):
    any_spec = pl.BlockSpec(memory_space=pl.ANY)
    dma = pltpu.SemaphoreType.DMA
    return pl.pallas_call(
        lookup_kernel,
        out_shape=[
            jax.ShapeDtypeStruct(hot_rows.shape, hot_rows.dtype),
            jax.ShapeDtypeStruct(cold_send.shape, cold_send.dtype),
            jax.ShapeDtypeStruct((N_DEV,) + vecs.shape, vecs.dtype),
        ],
        in_specs=[any_spec] * 3,
        out_specs=[any_spec] * 3,
        scratch_shapes=[dma((2, LOOK_N))] * 3 + [dma((N_DEV - 1,))] * 4 + [dma((2,))],
        input_output_aliases={1: 0},
        compiler_params=pltpu.CompilerParams(collective_id=0, has_side_effects=True),
        name="lookup_exchange",
    )(cold_send, hot_rows, vecs)


def pick_kernel(idx_ref, hot_ref, cold_ref, gain_ref, x_ref, hid_ref, inv_ref, rows, picked, sem):
    step = pl.program_id(0)
    count, width = x_ref.shape
    base = step * count

    @pl.when(step == 0)
    def _():
        hot = pltpu.make_async_copy(hot_ref, rows.at[pl.ds(0, HOT)], sem.at[0])
        cold = pltpu.make_async_copy(cold_ref, rows.at[pl.ds(HOT, cold_ref.shape[0])], sem.at[1])
        hot.start()
        cold.start()
        hot.wait()
        cold.wait()

    def body(i8, carry):
        for j in range(8):
            i = i8 * 8 + j
            picked[i] = rows[idx_ref[base + i]]
        return carry

    lax.fori_loop(0, count // 8, body, 0)
    x = picked[...].reshape(count, width)
    x_ref[...] = x
    x_full = x.astype(jnp.float32)
    inv = lax.rsqrt(jnp.mean(x_full * x_full, axis=-1, keepdims=True) + NORM_EPS)
    inv_ref[...] = inv
    hid_ref[...] = (x_full * inv * gain_ref[...]).astype(jnp.bfloat16)


def pick_rows(idx, hot, cold, gain, block):
    count = idx.shape[0]
    tail = hot.shape[1:]
    width = tail[0] * tail[1]
    any_spec = pl.BlockSpec(memory_space=pl.ANY)
    wide = pl.BlockSpec((block, width), lambda i, s: (i, 0))
    act = jax.ShapeDtypeStruct((count, width), hot.dtype)
    return pl.pallas_call(
        pick_kernel,
        grid_spec=pltpu.PrefetchScalarGridSpec(
            num_scalar_prefetch=1,
            grid=(count // block,),
            in_specs=[any_spec, any_spec, pl.BlockSpec((1, width), lambda i, s: (0, 0))],
            out_specs=[wide, wide, pl.BlockSpec((block, 1), lambda i, s: (i, 0))],
            scratch_shapes=[
                pltpu.VMEM((hot.shape[0] + cold.shape[0],) + tail, hot.dtype),
                pltpu.VMEM((block,) + tail, hot.dtype),
                pltpu.SemaphoreType.DMA((2,)),
            ],
        ),
        out_shape=[act, act, jax.ShapeDtypeStruct((count, 1), jnp.float32)],
        compiler_params=pltpu.CompilerParams(dimension_semantics=("arbitrary",), vmem_limit_bytes=VMEM_MAX),
        name="pick_rows",
    )(idx, hot, cold, gain)


def take2d_kernel(idx_ref, idx2_ref, rows_ref, out_ref, out2_ref, buf):
    step = pl.program_id(0)

    def copy_rows(idx, dst, count):
        def body(i8, carry):
            for j in range(8):
                i = i8 * 8 + j
                dst[pl.ds(i, 1), :] = rows_ref[pl.ds(idx[step * count + i], 1), :]
            return carry

        lax.fori_loop(0, count // 8, body, 0)

    copy_rows(idx_ref, buf, buf.shape[0])
    out_ref[...] = buf[...].astype(out_ref.dtype)
    copy_rows(idx2_ref, out2_ref, out2_ref.shape[0])


def take2d(idx, idx2, rows, steps):
    count, count2 = idx.shape[0] // steps, idx2.shape[0] // steps
    width = rows.shape[1]
    return pl.pallas_call(
        take2d_kernel,
        grid_spec=pltpu.PrefetchScalarGridSpec(
            num_scalar_prefetch=2,
            grid=(steps,),
            in_specs=[pl.BlockSpec(rows.shape, lambda i, a, b: (0, 0), pipeline_mode=pl.Buffered(1))],
            out_specs=[
                pl.BlockSpec((count, width), lambda i, a, b: (i, 0)),
                pl.BlockSpec((count2, width), lambda i, a, b: (i, 0)),
            ],
            scratch_shapes=[pltpu.VMEM((count, width), jnp.float32)],
        ),
        out_shape=[
            jax.ShapeDtypeStruct((count * steps, width), jnp.bfloat16),
            jax.ShapeDtypeStruct((count2 * steps, width), jnp.float32),
        ],
        compiler_params=pltpu.CompilerParams(dimension_semantics=("arbitrary",), vmem_limit_bytes=VMEM_MAX),
        name="take_rows",
    )(idx, idx2, rows)


def seg_sum_kernel(key_ref, off_ref, mine_ref, mate_ref, out_ref, src, sem):
    blk = pl.program_id(0)
    count = mine_ref.shape[0]

    @pl.when(blk == 0)
    def _():
        first = pltpu.make_async_copy(mine_ref, src.at[pl.ds(0, count)], sem.at[0])
        second = pltpu.make_async_copy(mate_ref, src.at[pl.ds(count, count)], sem.at[1])
        first.start()
        second.start()
        first.wait()
        second.wait()

    out_ref[...] = jnp.zeros_like(out_ref)

    def body(e, carry):
        key = key_ref[e]
        row = lax.shift_right_logical(key, 12) - blk * ROW_BLOCK
        tok = jnp.bitwise_and(key, 4095)
        out_ref[pl.ds(row, 1), :] += src[pl.ds(tok, 1), :]
        return carry

    lax.fori_loop(off_ref[blk], off_ref[blk + 1], body, 0)


def seg_sum(keys, offs, dx_mine, dx_mate, n_rows):
    tokens, width = dx_mine.shape
    any_spec = pl.BlockSpec(memory_space=pl.ANY)
    return pl.pallas_call(
        seg_sum_kernel,
        grid_spec=pltpu.PrefetchScalarGridSpec(
            num_scalar_prefetch=2,
            grid=(n_rows // ROW_BLOCK,),
            in_specs=[any_spec, any_spec],
            out_specs=pl.BlockSpec((ROW_BLOCK, width), lambda i, a, b: (i, 0)),
            scratch_shapes=[pltpu.VMEM((2 * tokens, width), jnp.float32), pltpu.SemaphoreType.DMA((2,))],
        ),
        out_shape=jax.ShapeDtypeStruct((n_rows, width), jnp.float32),
        compiler_params=pltpu.CompilerParams(dimension_semantics=("arbitrary",), vmem_limit_bytes=VMEM_MAX),
        name="hot_seg_sum",
    )(keys, offs, dx_mine, dx_mate)


RED_CHUNK = 32
RED_N = HOT // 2 // RED_CHUNK


def reduce_kernel(part_ref, cold_ref, more_ref, vec_ref, hot_ref, crecv_ref, mrecv_ref, vrecv_ref,
                  local, incoming, load_sem, send_sem, recv_sem, out_sem,
                  c_send, c_recv, m_send, m_recv, v_send, v_recv, l_sem):
    me = lax.axis_index(AXIS)
    chip, core = me // 2, me % 2
    mid = jnp.where(core == 0, 1, 2)
    first = 3 - mid
    place = jnp.where(chip == first, 0, jnp.where(chip == 3, 1, jnp.where(chip == mid, 2, 3)))
    nxt = jnp.where(chip == first, 3, jnp.where(chip == 3, mid, 0))
    target = nxt * 2 + core

    def rows(k):
        return pl.ds(k * RED_CHUNK, RED_CHUNK)

    def load(k):
        return pltpu.make_async_copy(part_ref.at[rows(k)], local.at[rows(k)], load_sem.at[k])

    def send(k):
        return pltpu.make_async_remote_copy(
            src_ref=local.at[rows(k)], dst_ref=incoming.at[rows(k)], send_sem=send_sem.at[k],
            recv_sem=recv_sem.at[k], device_id=(target,), device_id_type=MESH)

    def put_own(k):
        return pltpu.make_async_copy(local.at[rows(k)], hot_ref.at[rows(k)], send_sem.at[k])

    def put_far(k):
        return pltpu.make_async_remote_copy(
            src_ref=local.at[rows(k)], dst_ref=hot_ref.at[pl.ds(HOT // 2 + k * RED_CHUNK, RED_CHUNK)],
            send_sem=send_sem.at[k], recv_sem=out_sem.at[k], device_id=(jnp.bitwise_xor(me, 1),), device_id_type=MESH)

    swaps = (
        (vec_ref, vrecv_ref, v_send, v_recv),
        (more_ref, mrecv_ref, m_send, m_recv),
        (cold_ref, crecv_ref, c_send, c_recv),
    )

    def swap(which, step):
        src, dst, s_sem, r_sem = swaps[which]
        peer = jnp.bitwise_xor(me, step)
        return pltpu.make_async_remote_copy(
            src_ref=src.at[peer], dst_ref=dst.at[me], send_sem=s_sem.at[step - 1], recv_sem=r_sem.at[step - 1],
            device_id=(peer,), device_id_type=MESH)

    def keep(which):
        src, dst, _, _ = swaps[which]
        return pltpu.make_async_copy(src.at[me], dst.at[me], l_sem.at[which])

    def start_load(k, carry):
        load(k).start()
        return carry

    lax.fori_loop(0, RED_N, start_load, 0)
    barrier_all(me)
    for which in range(3):
        keep(which).start()
    for which in range(2):
        for step in range(1, N_DEV):
            swap(which, step).start()

    def cold_at(k, step):
        return jnp.where(place >= 2, k == 0, k == 4 * step)

    def stage(k, carry):
        @pl.when(k < RED_N)
        def _():
            load(k).wait()

        @pl.when((k < RED_N) & (place > 0))
        def _():
            send(k).wait_recv()
            local[rows(k), :] += incoming[rows(k), :]

        @pl.when((k >= 1) & (place < 3))
        def _():
            send(k - 1).start()

        for step in range(1, N_DEV):
            @pl.when(cold_at(k, step))
            def _():
                swap(2, step).start()

        @pl.when((k >= 1) & (me == 0))
        def _():
            put_own(k - 1).start()

        @pl.when((k >= 1) & (me == 1))
        def _():
            put_far(k - 1).start()
        return carry

    lax.fori_loop(0, RED_N + 1, stage, 0)

    def drain(k, carry):
        @pl.when(place < 3)
        def _():
            send(k).wait_send()

        @pl.when(me == 0)
        def _():
            put_own(k).wait()
            put_far(k).wait_recv()

        @pl.when(me == 1)
        def _():
            put_far(k).wait_send()
        return carry

    lax.fori_loop(0, RED_N, drain, 0)
    for which in range(3):
        for step in range(1, N_DEV):
            swap(which, step).wait()
        keep(which).wait()


def grad_exchange(part, cold_send, more_send, vecs):
    any_spec = pl.BlockSpec(memory_space=pl.ANY)
    dma = pltpu.SemaphoreType.DMA
    width = part.shape[1]
    return pl.pallas_call(
        reduce_kernel,
        out_shape=[jax.ShapeDtypeStruct((HOT, width), jnp.float32)]
        + [jax.ShapeDtypeStruct(a.shape, a.dtype) for a in (cold_send, more_send, vecs)],
        in_specs=[any_spec] * 4,
        out_specs=[any_spec] * 4,
        scratch_shapes=[pltpu.VMEM(part.shape, jnp.float32)] * 2
        + [dma((RED_N,))] * 4 + [dma((N_DEV - 1,))] * 6 + [dma((3,))],
        compiler_params=pltpu.CompilerParams(
            collective_id=1, has_side_effects=True, vmem_limit_bytes=VMEM_MAX),
        name="grad_exchange",
    )(part, cold_send, more_send, vecs)


def table_kernel(key_ref, off_ref, n_hot_ref, src_ref, more_ref, hot_ref, out_ref, acc, rows, half_rows, sem):
    blk = pl.program_id(0)
    n_src = src_ref.shape[0]

    @pl.when(blk == 0)
    def _():
        low = pltpu.make_async_copy(src_ref, half_rows, sem.at[0])
        high = pltpu.make_async_copy(more_ref, rows.at[pl.ds(n_src, more_ref.shape[0])], sem.at[1])
        low.start()
        high.start()
        low.wait()
        for c in range(N_DEV):
            part = pl.ds(c * (n_src // N_DEV), n_src // N_DEV)
            rows[part, :] = half_rows[part, :].astype(jnp.float32)
        high.wait()

    is_hot = blk < n_hot_ref[0]

    @pl.when(is_hot)
    def _():
        acc[...] = hot_ref[...]

    @pl.when(jnp.logical_not(is_hot))
    def _():
        acc[...] = jnp.zeros_like(acc)

    def body(e, carry):
        key = key_ref[e]
        row = lax.shift_right_logical(key, 11) - blk * TABLE_BLOCK
        idx = jnp.bitwise_and(key, 2047)
        acc[pl.ds(row, 1), :] += rows[pl.ds(idx, 1), :]
        return carry

    lax.fori_loop(off_ref[blk], off_ref[blk + 1], body, 0)
    out_ref[...] = acc[...].astype(out_ref.dtype)


def build_table(keys, offs, n_hot, src, more, hot, n_rows):
    width = src.shape[1]

    def hot_index(i, k, o, n):
        return (jnp.minimum(i, jnp.maximum(n[0] - 1, 0)), 0)

    return pl.pallas_call(
        table_kernel,
        grid_spec=pltpu.PrefetchScalarGridSpec(
            num_scalar_prefetch=3,
            grid=(pl.cdiv(n_rows, TABLE_BLOCK),),
            in_specs=[
                pl.BlockSpec(memory_space=pl.ANY),
                pl.BlockSpec(memory_space=pl.ANY),
                pl.BlockSpec((TABLE_BLOCK, width), hot_index),
            ],
            out_specs=pl.BlockSpec((TABLE_BLOCK, width), lambda i, k, o, n: (i, 0)),
            scratch_shapes=[
                pltpu.VMEM((TABLE_BLOCK, width), jnp.float32),
                pltpu.VMEM((src.shape[0] + more.shape[0], width), jnp.float32),
                pltpu.VMEM(src.shape, src.dtype),
                pltpu.SemaphoreType.DMA((2,)),
            ],
        ),
        out_shape=jax.ShapeDtypeStruct((n_rows, width), jnp.bfloat16),
        compiler_params=pltpu.CompilerParams(dimension_semantics=("arbitrary",), vmem_limit_bytes=VMEM_MAX),
        name="build_table",
    )(keys, offs, n_hot, src, more, hot)


def lookup_plan(all_ids, own_ids, me, rows_dev):
    tokens = own_ids.shape[0]
    t_idx = jnp.arange(tokens, dtype=jnp.int32)
    devices = jnp.arange(N_DEV, dtype=jnp.int32)
    first_row = me * rows_dev
    mine = (all_ids >= HOT) & (all_ids >= first_row) & (all_ids < first_row + rows_dev)
    key = first_of(mine, t_idx[None, :] * 32768 + (all_ids - first_row), CAP)
    ask_row = jnp.where(key != BIG, jnp.bitwise_and(key, 32767), 0).reshape(-1)
    hit = (own_ids // rows_dev == devices[:, None]) & (own_ids >= HOT)[None, :]
    place = jnp.cumsum(hit.astype(jnp.int32), axis=1) - 1 + devices[:, None] * CAP
    idx = jnp.where(own_ids >= HOT, HOT + jnp.sum(jnp.where(hit, place, 0), axis=0), own_ids)
    return ask_row, idx


def fast_lookup(ask_row, idx, table_part, gain_vecs):
    width = table_part.shape[1]
    send = jnp.take(table_part, ask_row, axis=0, mode="clip")
    tiles = (width // LANES, LANES)
    send = send.reshape((N_DEV, CAP) + tiles)
    hot, cold, vecs = lookup_exchange(send, table_part[:HOT].reshape((HOT,) + tiles), gain_vecs)
    vecs = vecs.transpose(1, 0, 2).reshape(gain_vecs.shape[0], -1).astype(jnp.float32)
    normed = pick_rows(idx, hot, cold.reshape((N_DEV * CAP,) + tiles), vecs[:1], 256)
    return normed, cold, vecs


def first_of(mask, values, count):
    return lax.sort(jnp.where(mask, values, BIG), dimension=1, is_stable=False)[:, :count]


def sort_rows(keys):
    keys = jnp.pad(keys, (0, max(0, 2048 - keys.shape[0])), constant_values=BIG)
    fill = jnp.full((7,) + keys.shape, BIG, jnp.int32)
    return lax.sort(jnp.concatenate([keys[None], fill]), dimension=1, is_stable=False)[0]


def repeats(all_ids):
    flat = all_ids.reshape(-1).astype(jnp.uint32)
    pos = jnp.arange(flat.shape[0], dtype=jnp.uint32)
    ordered = lax.sort(flat * jnp.uint32(16384) + pos, is_stable=False)
    ident = ordered // jnp.uint32(16384)
    same = ident[1:] == ident[:-1]
    no = jnp.zeros((1,), jnp.bool_)
    again = jnp.concatenate([no, same]) | jnp.concatenate([same, no])
    again = lax.sort((ordered % jnp.uint32(16384)) * jnp.uint32(2) + again.astype(jnp.uint32), is_stable=False) % jnp.uint32(2)
    return (again == 1).reshape(all_ids.shape)


def grad_plan(all_ids, own_ids, again, me, rows_dev):
    tokens = own_ids.shape[0]
    t_idx = jnp.arange(tokens, dtype=jnp.int32)[None, :]
    devices = jnp.arange(N_DEV, dtype=jnp.int32)
    owners = jnp.where(all_ids >= HOT, all_ids // rows_dev, -1)
    hit = lax.dynamic_index_in_dim(owners, me, 0, keepdims=False)[None, :] == devices[:, None]
    own_again = lax.dynamic_index_in_dim(again, me, 0, keepdims=True)
    slot_tok = first_of(hit, t_idx, CAP)
    more_tok = first_of(hit & own_again, t_idx, MORE)
    mine = owners == me
    local = all_ids - me * rows_dev
    row = first_of(mine, t_idx * 65536 + local * 2 + again, CAP)
    more_row = first_of(mine & again, t_idx * 65536 + local * 2 + again, MORE)
    slots = jnp.arange(N_DEV * CAP, dtype=jnp.int32).reshape(N_DEV, CAP)
    more_slots = N_DEV * CAP + jnp.arange(N_DEV * MORE, dtype=jnp.int32).reshape(N_DEV, MORE)

    def owner_key(packed, slot, wanted):
        where = jnp.bitwise_and(lax.shift_right_logical(packed, 1), 32767)
        return jnp.where((packed != BIG) & (jnp.bitwise_and(packed, 1) == wanted), where * 2048 + slot, BIG).reshape(-1)

    owner_keys = sort_rows(jnp.concatenate([owner_key(row, slots, 0), owner_key(more_row, more_slots, 1)]))
    mate_ids = lax.dynamic_index_in_dim(all_ids, jnp.bitwise_xor(me, 1), 0, keepdims=False)
    pair_ids = jnp.concatenate([own_ids, mate_ids])
    base = (me % 2) * (HOT // 2)
    inside = (pair_ids >= base) & (pair_ids < base + HOT // 2)
    hot_keys = jnp.where(inside, (pair_ids - base) * 4096 + jnp.arange(2 * tokens, dtype=jnp.int32), BIG)
    hot_keys = sort_rows(hot_keys)

    def clean(tok):
        return jnp.where(tok == BIG, 0, tok).reshape(-1)

    return clean(slot_tok), clean(more_tok), owner_keys, hot_keys


def block_offsets(keys, n_blocks, block, shift):
    edges = jnp.arange(n_blocks + 1, dtype=jnp.int32) * (block << shift)
    return jnp.sum(keys[None, :] < edges[:, None], axis=1).astype(jnp.int32)


def fast_table_grad(rows_dev, d_x, vecs, slot_tok, more_tok, owner_keys, keys):
    tokens, width = d_x.shape
    me = lax.axis_index(AXIS)
    mate_of = [(i, i ^ 1) for i in range(N_DEV)]
    dx_mate = lax.ppermute(d_x, AXIS, mate_of)
    part = seg_sum(keys, block_offsets(keys, HOT // 2 // ROW_BLOCK, ROW_BLOCK, 12), d_x, dx_mate, HOT // 2)
    cold, more = take2d(slot_tok, more_tok, d_x, N_DEV)
    cold = cold.reshape(N_DEV, CAP, width)
    more = more.reshape(N_DEV, MORE, width)
    hot, recv, more_recv, vec_recv = grad_exchange(part, cold, more, vecs)
    n_hot = jnp.where(me == 0, HOT // TABLE_BLOCK, 0).astype(jnp.int32)[None]
    offs = block_offsets(owner_keys, pl.cdiv(rows_dev, TABLE_BLOCK), TABLE_BLOCK, 11)
    recv = recv.reshape(N_DEV * CAP, width)
    more_recv = more_recv.reshape(N_DEV * MORE, width)
    grad_part = build_table(owner_keys, offs, n_hot, recv, more_recv, hot, rows_dev)
    return grad_part, jnp.sum(vec_recv, axis=0)


def slow_lookup(all_ids, table_part, me):
    rows_dev = table_part.shape[0]
    local_idx = all_ids - me * rows_dev
    is_owned = (local_idx >= 0) & (local_idx < rows_dev)
    looked = jnp.take(table_part, jnp.where(is_owned, local_idx, 0), axis=0)
    looked = jnp.where(is_owned[..., None], looked, jnp.zeros((), jnp.bfloat16))
    return lax.psum_scatter(looked, AXIS, scatter_dimension=0)


def slow_table_grad(rows_dev, all_ids, d_x, vecs):
    me = lax.axis_index(AXIS)
    local_idx = all_ids - me * rows_dev
    is_owned = (local_idx >= 0) & (local_idx < rows_dev)
    all_dx = lax.all_gather(d_x, AXIS)
    seg_idx = jnp.where(is_owned, local_idx, rows_dev)
    grad_part = jax.ops.segment_sum(all_dx.reshape(-1, d_x.shape[-1]), seg_idx.reshape(-1), num_segments=rows_dev)
    return grad_part.astype(jnp.bfloat16), lax.psum_scatter(vecs, AXIS, scatter_dimension=0)


def solution(mesh):
    row_spec = P(AXIS, None)
    vec_spec = P(AXIS)
    act_spec = P(AXIS, None, None)
    weight_specs = (vec_spec, row_spec, vec_spec, row_spec, vec_spec, row_spec, vec_spec, row_spec)
    in_specs = (row_spec, act_spec, row_spec) + weight_specs
    out_specs = (act_spec, row_spec) + weight_specs

    def run(fast, tok_ids, all_ids, again, ask_row, idx, grad_out, table_part, gain_part, wq_part, bq_part, wk_part, bk_part, wv_part, bv_part, wo_part):
        me = lax.axis_index(AXIS)
        rows_dev, width = table_part.shape
        n_seq, seq_len = tok_ids.shape
        own_ids = tok_ids.reshape(-1)

        def whole(part):
            return lax.all_gather(part, AXIS, axis=0, tiled=True)

        def scatter(grad):
            return lax.psum_scatter(grad, AXIS, scatter_dimension=0, tiled=True)

        part_w = gain_part.shape[0]
        group = wq_part.shape[1] // GROUPS
        cols = [slice(g * group, (g + 1) * group) for g in range(GROUPS)]
        vec_parts = jnp.pad(jnp.stack([gain_part, bq_part, bk_part, bv_part]), ((0, 12), (0, 0)))
        w_parts = [jnp.concatenate([wq_part[:, c], wk_part[:, c], wv_part[:, c]], axis=1) for c in cols]
        if fast:
            (x_rows, hidden, inv_rms), marker, vec_full = fast_lookup(ask_row, idx, table_part, vec_parts)
            late = lax.optimization_barrier((marker, all_ids, own_ids, again, wo_part, *w_parts[1:]))
            plan_ids, wo_part, w_parts = late[1:4], late[4], [w_parts[0], *late[5:]]
        else:
            x_rows = slow_lookup(all_ids, table_part, me)
            vec_full = lax.all_gather(vec_parts, AXIS, axis=1, tiled=True).astype(jnp.float32)
            x_full = x_rows.astype(jnp.float32)
            inv_rms = lax.rsqrt(jnp.mean(x_full * x_full, axis=-1, keepdims=True) + NORM_EPS)
            hidden = (x_full * inv_rms * vec_full[0]).astype(jnp.bfloat16)
        biases = [jnp.concatenate([vec_full[1, c], vec_full[2, c], vec_full[3, c]])[None] for c in cols]
        wo_full = whole(wo_part)
        w_groups = [whole(part) for part in w_parts]
        grad_flat = grad_out.reshape(-1, width)
        block_out, d_x, grad_ws, grad_wo, grad_gain, grad_bias = block_fwd_bwd(
            x_rows, hidden, inv_rms, grad_flat, seq_len, vec_full[0], biases, w_groups, wo_full, scatter)
        gq, gk, gv = (
            jnp.concatenate([grad_w[:, j * group:(j + 1) * group] for grad_w in grad_ws], axis=1) for j in range(3))
        grad_bias = grad_bias.reshape(GROUPS, 3, group)
        vecs = jnp.stack([grad_gain] + [grad_bias[:, j].reshape(-1) for j in range(3)])
        vecs = jnp.pad(vecs.reshape(4, N_DEV, part_w).transpose(1, 0, 2), ((0, 0), (0, 4), (0, 0)))
        if fast:
            grad_part, vec_sum = fast_table_grad(rows_dev, d_x, vecs, *grad_plan(*plan_ids, me, rows_dev))
        else:
            grad_part, vec_sum = slow_table_grad(rows_dev, all_ids, d_x, vecs)
        return (block_out.reshape(grad_out.shape), grad_part, vec_sum[0], gq, vec_sum[1], gk, vec_sum[2], gv, vec_sum[3], grad_wo)

    def device_step(tok_ids, grad_out, table_part, *weights):
        rows_dev = table_part.shape[0]
        all_ids = lax.all_gather(tok_ids.reshape(-1), AXIS)
        me = lax.axis_index(AXIS)
        again = repeats(all_ids)
        owners = jnp.where(all_ids >= HOT, all_ids // rows_dev, -1)
        asked = owners[None] == jnp.arange(N_DEV, dtype=jnp.int32)[:, None, None]
        counts = jnp.sum(asked.astype(jnp.int32), axis=-1)
        more = jnp.sum((asked & again[None]).astype(jnp.int32), axis=-1)
        fits = (jnp.max(counts) <= CAP) & (jnp.max(more) <= MORE)
        ask_row, idx = lookup_plan(all_ids, tok_ids.reshape(-1), me, rows_dev)
        args = (tok_ids, all_ids, again, ask_row, idx, grad_out, table_part) + weights
        return lax.cond(fits, functools.partial(run, True), functools.partial(run, False), *args)

    return jax.shard_map(device_step, mesh=mesh, in_specs=in_specs, out_specs=out_specs, check_vma=False)
```
